32 devices in a mesh: row: 4 (over y, core), col: 8 (over z, x).
Axes of the slice: x: 2, y: 2, z: 4, core: 2. Of those that a mesh axis runs over, the one named last changes fastest.
Arguments:
- parent_front: float32 [8, 1024, 4, 2048], P(None, 'row', None, 'col'), may hold values from -6 to 6
- generators: bfloat16 [48, 256, 256], P('row'), may hold values from -1.5 to 1.5
- diagonal_blocks: bfloat16 [48, 256, 256], P('row'), may hold values from -6 to 6
- coupling: bfloat16 [2, 256, 256], replicated, may hold values from -0.375 to 0.375
- block_map: int32 [2, 24], replicated, may hold values from 0 to 31, as said below
- valid_rows: int32 [2, 24], replicated, may hold values from 128 to 256
Outputs:
- assembled: float32 [8, 1024, 4, 2048], P(None, 'row', None, 'col')
The draws below stay inside these ranges and needn't reach their ends.
Inputs may be any that keep to these rules, and one draw needn't show every extreme that they name: `block_map`: for each child c and each s < 2, the child blocks s * 12 to (s + 1) * 12 - 1 map in increasing order to distinct parent blocks of the range s * 16 to (s + 1) * 16 - 1, and the parent blocks s * 16 + m * 4 of that range always receive one.
All inputs are finite; a program needn't handle non-finite values.
Results may differ from the reference program's by a relative error of at most 0.0028.
Values may be sent and summed in bfloat16 or wider, within the bound.
No kernel may reach another device: no remote copies, remote signals or barrier semaphores. Data moves between devices by JAX's collectives and lax.ppermute only.
A program may use at most 128 MiB of HBM per device.

```python
import jax
import jax.numpy as jnp
from jax import lax

BLK = 256
RANK = 256
BR_DEV = 8
PB = 32
BC_DEV = 4
WIN = 16
CG = 12
HALF = 2
CB = 24
N_ROW = 4
N_COL = 8


def draw_block_map(key, part):
    child_rows = []
    for child_index in range(2):
        pieces = []
        for group_index in range(HALF):
            window_key = jax.random.fold_in(key, 1000 * child_index + group_index + 17)
            offsets = jnp.arange(WIN, dtype=jnp.int32)
            scores = jax.random.randint(window_key, (WIN,), 0, 1 << 20, dtype=jnp.int32) * WIN + offsets
            scores = jnp.where(offsets % N_ROW == 0, jnp.int32(1 << 30), scores)
            gap_order = jnp.argsort(scores, stable=True)
            gap_slots = gap_order[:WIN - CG]
            gap_flags = jnp.zeros((WIN,), jnp.int32).at[gap_slots].set(1)
            sorted_slots = jnp.argsort(gap_flags * WIN + offsets, stable=True).astype(jnp.int32)
            chosen = sorted_slots[:CG] + WIN * group_index
            pieces.append(chosen)
        child_rows.append(jnp.concatenate(pieces))
    return jnp.stack(child_rows).astype(jnp.int32)


def place_ends(entries, own_key, low, high):
    longest = entries.shape.index(max(entries.shape))
    spots = []
    for shift in (0, 1):
        where = [jax.random.randint(jax.random.fold_in(own_key, axis), (), 0, length) for axis, length in enumerate(entries.shape)]
        where[longest] = (where[longest] + shift) % entries.shape[longest]
        spots.append(tuple(where))
    return entries.at[spots[0]].set(low).at[spots[1]].set(high)


def shard_levels(own_key, extent, cuts, smallest, largest):
    def one(dim, blocks):
        heights = jax.random.uniform(jax.random.fold_in(jax.random.fold_in(own_key, 6), dim), (blocks,), jnp.float32, smallest / len(cuts), largest / len(cuts))
        return jnp.repeat(jnp.exp(heights), extent[dim] // blocks).reshape((-1,) + (1,) * (len(extent) - dim - 1))

    loudness = one(*cuts[0])
    for cut in cuts[1:]:
        loudness = loudness * one(*cut)
    return loudness


def bell_draw(stream_key, dims, scale, reach, cuts=(), held_as=jnp.bfloat16):
    entries = jax.random.normal(stream_key, dims, jnp.float32) * scale
    if len(cuts) > 0:
        entries = shard_levels(stream_key, dims, cuts, -0.22, 0.18) * entries
    return jnp.clip(entries, min=-reach, max=reach).astype(held_as)


def setup_inputs(seed: int = 0) -> dict:
    arg_keys = jax.random.split(jax.random.key(seed), 7)
    parent_front = bell_draw(arg_keys[0], (BR_DEV, N_ROW * BLK, BC_DEV, N_COL * BLK), 1.0, 6.0, ((1, 4), (3, 8)), jnp.float32)
    generators = bell_draw(arg_keys[1], (2 * CB, BLK, RANK), 0.25, 1.5, ((0, 4),))
    diagonal_blocks = bell_draw(arg_keys[2], (2 * CB, BLK, BLK), 1.0, 6.0, ((0, 4),))
    coupling = bell_draw(arg_keys[3], (2, RANK, RANK), RANK ** -0.5, 0.375)
    block_map = draw_block_map(jax.random.fold_in(arg_keys[6], 71), 0)
    valid_rows = place_ends(jax.random.randint(arg_keys[5], (2, CB), BLK // 2, BLK + 1), jax.random.fold_in(arg_keys[5], 1), BLK // 2, BLK).astype(jnp.int32)
    return dict(parent_front=parent_front, generators=generators, diagonal_blocks=diagonal_blocks, coupling=coupling, block_map=block_map, valid_rows=valid_rows)


def child_select(stacked, child_index):
    grouped = stacked.reshape((HALF, 2, CG) + stacked.shape[1:])
    return grouped[:, child_index].reshape((CB,) + stacked.shape[1:])


def child_parts(gen_blocks, diag_rows, coupling_one, map_row, count_row):
    row_offsets = jnp.arange(BLK, dtype=jnp.int32)
    kept_mask = (row_offsets[None, :] < count_row[:, None]).astype(jnp.float32)
    masked = gen_blocks.astype(jnp.float32) * kept_mask[:, :, None]
    projected = jnp.einsum("ixq,qr->ixr", masked, coupling_one.astype(jnp.float32)).astype(jnp.bfloat16)
    diag_kept = diag_rows.astype(jnp.float32) * kept_mask[:, :, None] * kept_mask[:, None, :]
    placing = (map_row[None, :] == jnp.arange(PB, dtype=jnp.int32)[:, None]).astype(jnp.float32)
    placed_gen = jnp.einsum("pi,ixq->pxq", placing, masked)
    placed_proj = jnp.einsum("pi,ixq->pxq", placing, projected.astype(jnp.float32))
    placed_diag = jnp.einsum("pi,ixz->pxz", placing, diag_kept)
    return placed_gen, placed_proj, placed_diag


def reference(parent_front, generators, diagonal_blocks, coupling, block_map, valid_rows):
    front_blocks = parent_front.reshape(PB, BLK, PB, BLK)
    child_data = [child_parts(child_select(generators, child_index),
                              child_select(diagonal_blocks, child_index),
                              coupling[child_index], block_map[child_index], valid_rows[child_index])
                  for child_index in range(2)]
    placed_gen = jnp.stack([child_data[0][0], child_data[1][0]], axis=1)
    placed_proj = jnp.stack([child_data[0][1], child_data[1][1]])
    placed_diag = jnp.stack([child_data[0][2], child_data[1][2]], axis=1)
    block_ids = jnp.arange(PB, dtype=jnp.int32)

    def one_row(row_items):
        front_row, gen_row, diag_row, row_id = row_items
        on_diag = (block_ids == row_id).astype(jnp.float32)
        running = front_row
        for child_index in range(2):
            child_tile = jnp.einsum("xq,jzq->xjz", gen_row[child_index], placed_proj[child_index])
            child_tile = child_tile + diag_row[child_index][:, None, :] * on_diag[None, :, None]
            rounded = lax.optimization_barrier(child_tile.astype(jnp.bfloat16))
            running = running + rounded.astype(jnp.float32)
        return running

    rows_out = lax.map(one_row, (front_blocks, placed_gen, placed_diag, block_ids))
    return rows_out.reshape(BR_DEV, N_ROW * BLK, BC_DEV, N_COL * BLK)
```

```python
import functools

import jax
import jax.numpy as jnp
from jax import lax
from jax.experimental import pallas as pl
from jax.experimental.pallas import tpu as pltpu
from jax.sharding import PartitionSpec as P


ANY = pl.BlockSpec(memory_space=pl.ANY)
SMEM = pl.BlockSpec(memory_space=pltpu.SMEM)
VMEM = pl.BlockSpec(memory_space=pltpu.VMEM)
LANES = 128


def in_hbm(x):
    return pltpu.with_memory_space_constraint(x, pltpu.HBM)


def place():
    row, col = lax.axis_index("row"), lax.axis_index("col")
    return row, col, row // 2, row % 2


def pack_kernel(dims, block_map, valid_rows, generators, diagonal, coupling, *refs):
    rows_n, cols_n, window = dims
    halves = rows_n // 2
    row_cap, col_cap = window // rows_n, window // cols_n
    flows = [(d, k) for d in range(halves) for k in range(2)][1:]
    row_out = dict(zip(flows, refs[: len(flows)]))
    col_out, diag_out, where, count, picked, mixer, sems = refs[len(flows):]
    row, col, group, child = place()
    group_blocks = generators.shape[0]
    block = generators.shape[1]

    mix = pltpu.make_async_copy(coupling.at[child], mixer, sems.at[0])
    mix.start()
    for slot in range(window):
        where[slot] = 0
        count[slot] = 0
    for i in range(group_blocks):
        spot = block_map[child, group * group_blocks + i] - group * window
        where[spot] = i
        count[spot] = valid_rows[child, group * group_blocks + i]

    loads, copies = [], []
    sem = 1
    for q in range(col_cap):
        source = where[q * cols_n + col]
        load = pltpu.make_async_copy(generators.at[source], picked.at[q], sems.at[sem])
        load.start()
        loads.append(load)
        sem += 1
    for (d, k) in reversed(flows):
        target = 2 * lax.rem(group + halves - d, halves) + (child + k) % 2
        for q in range(row_cap):
            source = where[q * rows_n + target]
            copy = pltpu.make_async_copy(
                generators.at[source], row_out[d, k].at[q], sems.at[sem])
            copy.start()
            copies.append(copy)
            sem += 1
    for q in range(col_cap):
        source = where[q * cols_n + col]
        copy = pltpu.make_async_copy(diagonal.at[source], diag_out.at[q], sems.at[sem])
        copy.start()
        copies.append(copy)
        sem += 1
    mix.wait()
    for q in range(col_cap):
        loads[q].wait()
        keep = lax.broadcasted_iota(jnp.int32, (block, 1), 0) < count[q * cols_n + col]
        masked = jnp.where(keep, picked[q], jnp.zeros_like(picked[q]))
        product = jnp.dot(masked, mixer[...], preferred_element_type=jnp.float32)
        col_out[q] = product.astype(col_out.dtype)
    for copy in copies:
        copy.wait()


def pack(dims, block_map, valid_rows, generators, diagonal, coupling):
    rows_n, cols_n, window = dims
    halves = rows_n // 2
    row_cap, col_cap = window // rows_n, window // cols_n
    _, block, rank = generators.shape
    dt = generators.dtype
    flows = 2 * halves - 1
    out_shape = (
        [jax.ShapeDtypeStruct((row_cap, block, rank), dt)] * flows
        + [jax.ShapeDtypeStruct((col_cap, block, rank), dt),
           jax.ShapeDtypeStruct((col_cap, block, block), dt)]
    )
    sem_count = 1 + col_cap * 2 + flows * row_cap
    return pl.pallas_call(
        functools.partial(pack_kernel, dims),
        out_shape=out_shape,
        in_specs=[SMEM, SMEM, ANY, ANY, ANY],
        out_specs=[VMEM] * len(out_shape),
        scratch_shapes=[
            pltpu.SMEM((window,), jnp.int32),
            pltpu.SMEM((window,), jnp.int32),
            pltpu.VMEM((col_cap, block, rank), dt),
            pltpu.VMEM((rank, rank), dt),
            pltpu.SemaphoreType.DMA((sem_count,)),
        ],
        compiler_params=pltpu.CompilerParams(vmem_limit_bytes=12 << 20),
        name="pack",
    )(in_hbm(block_map), in_hbm(valid_rows), in_hbm(generators), in_hbm(diagonal), in_hbm(coupling))


def update_kernel(dims, d, block_map, valid_rows, left_a, left_b, diag_a, diag_b, *refs):
    rows_n, cols_n, window = dims
    halves = rows_n // 2
    row_cap, col_cap = window // rows_n, window // cols_n
    rights = refs[: 2 * halves]
    refs = refs[2 * halves:]
    if d > 0:
        front, _, out, count = refs
    else:
        front, out, count, where, left, diag, sems = refs
    row, col, group, child = place()
    aim = lax.rem(group + d, halves)
    block = left_b.shape[1]
    group_blocks = block_map.shape[1] // halves
    cols_local = halves * col_cap
    q = pl.program_id(0)

    def fetch(s):
        source = where[s * rows_n + row]
        return pltpu.make_async_copy(left_a.at[source], left.at[s], sems.at[s])

    def fetch_diag(s):
        source = where[s * cols_n + col]
        return pltpu.make_async_copy(diag_a.at[source], diag.at[s], sems.at[row_cap + s])

    @pl.when(q == 0)
    def _():
        for slot in range(window):
            if d == 0:
                where[slot] = 0
            for k in range(2):
                count[k, slot] = 0
        for k in range(2):
            who = (child + k) % 2
            for i in range(group_blocks):
                spot = block_map[who, aim * group_blocks + i] - aim * window
                count[k, spot] = valid_rows[who, aim * group_blocks + i]
                if d == 0 and k == 0:
                    where[spot] = i
        if d == 0:
            for s in range(row_cap):
                fetch(s).start()
            for s in range(col_cap):
                fetch_diag(s).start()
            for s in range(col_cap):
                fetch_diag(s).wait()

    if d == 0:
        fetch(q).wait()
        lefts = (left[q], left_b[q])
        diags = (diag, diag_b)
    else:
        lefts = (left_a[q], left_b[q])
        diags = (diag_a, diag_b)
    spot = q * rows_n + row
    x_pos = lax.broadcasted_iota(jnp.int32, (block, 1), 0)
    y_pos = lax.broadcasted_iota(jnp.int32, (1, block), 1)
    lefts = [jnp.where(x_pos < count[k, spot], lefts[k], jnp.zeros_like(lefts[k])) for k in range(2)]
    contract = (((1,), (1,)), ((), ()))
    step = 2 * cols_local
    for e in range(halves):
        for s in range(col_cap):
            b = lax.rem(group + e, halves) * col_cap + s
            total = sum(
                lax.dot_general(lefts[k], rights[2 * e + k][s], contract,
                                preferred_element_type=jnp.float32)
                for k in range(2))
            for part in range(block // LANES):
                rows = pl.ds(part * cols_local + b, block, stride=step)
                out[0, rows, :] = front[0, rows, :] + total[:, part * LANES:(part + 1) * LANES]
    offset = spot - col

    @pl.when(lax.rem(offset + cols_n * rows_n, cols_n) == 0)
    def _():
        s = (offset + cols_n) // cols_n - 1
        b = aim * col_cap + s
        extra = jnp.zeros((block, block), jnp.float32)
        for k in range(2):
            keep = (x_pos < count[k, spot]) & (y_pos < count[k, spot])
            extra += jnp.where(keep, diags[k][s].astype(jnp.float32), 0.0)
        for part in range(block // LANES):
            rows = pl.ds(part * cols_local + b, block, stride=step)
            out[0, rows, :] += extra[:, part * LANES:(part + 1) * LANES]


def update(dims, d, block_map, valid_rows, lefts, diags, rights, front, prior):
    rows_n, cols_n, window = dims
    halves = rows_n // 2
    row_cap, col_cap = window // rows_n, window // cols_n
    _, block, rank = lefts[0].shape
    dt = lefts[0].dtype

    def where_front(q):
        row = lax.axis_index("row")
        return (lax.rem(row // 2 + d, halves) * row_cap + q, 0, 0)

    view = pl.BlockSpec((1,) + front.shape[1:], where_front)
    own = ANY if d == 0 else VMEM
    if d == 0:
        lefts = (in_hbm(lefts[0]), lefts[1])
        diags = (in_hbm(diags[0]), diags[1])
    args = [in_hbm(block_map), in_hbm(valid_rows), *lefts, *diags, *rights, in_hbm(front)]
    specs = [SMEM, SMEM, own, VMEM, own, VMEM] + [VMEM] * len(rights) + [view]
    scratch = [pltpu.SMEM((2, window), jnp.int32)]
    aliases = {}
    if d > 0:
        aliases = {len(args): 0}
        args.append(prior)
        specs.append(ANY)
    else:
        scratch += [
            pltpu.SMEM((window,), jnp.int32),
            pltpu.VMEM((row_cap, block, rank), dt),
            pltpu.VMEM((col_cap, block, block), dt),
            pltpu.SemaphoreType.DMA((row_cap + col_cap,)),
        ]
    return pl.pallas_call(
        functools.partial(update_kernel, dims, d),
        out_shape=jax.ShapeDtypeStruct(front.shape, front.dtype),
        grid=(row_cap,),
        in_specs=specs,
        out_specs=view,
        input_output_aliases=aliases,
        scratch_shapes=scratch,
        compiler_params=pltpu.CompilerParams(vmem_limit_bytes=24 << 20),
        name=f"update{d}",
    )(*args)


def shards(rows_n, cols_n, parent_front, generators, diagonal_blocks, coupling, block_map, valid_rows):
    halves = rows_n // 2
    rows_local, block, cols_local, width = parent_front.shape
    window = 2 * rows_local
    dims = (rows_n, cols_n, window)
    parts = width // LANES

    front = parent_front.reshape(rows_local, block, cols_local, parts, LANES)
    front = front.transpose(0, 1, 3, 2, 4).reshape(rows_local, block * parts * cols_local, LANES)

    flows = [(d, k) for d in range(halves) for k in range(2)][1:]
    packed = pack(dims, block_map, valid_rows, generators, diagonal_blocks, coupling)
    row_send = dict(zip(flows, packed[: len(flows)]))
    col_own, diag_own = packed[len(flows):]

    def target(row, d, k):
        return 2 * ((row // 2 - d) % halves) + (row % 2 + k) % 2

    def send(x, d, k, only_diag=False):
        pairs = [
            (row * cols_n + col, target(row, d, k) * cols_n + col)
            for row in range(rows_n)
            for col in range(cols_n)
            if not only_diag or target(row, d, k) == col % rows_n
        ]
        return lax.ppermute(x, ("row", "col"), pairs)

    rights = {(0, 0): col_own}
    lefts = {(0, 0): generators}
    diags = {(0, 0): diagonal_blocks}
    for d, k in flows:
        rights[d, k] = send(col_own, d, k)
        lefts[d, k] = send(row_send[d, k], d, k)
        diags[d, k] = send(diag_own, d, k, True)
    out = None
    order = [rights[d, k] for d in range(halves) for k in range(2)]
    for d in range(halves):
        out = update(
            dims, d, block_map, valid_rows,
            (lefts[d, 0], lefts[d, 1]), (diags[d, 0], diags[d, 1]), order, front, out)
    out = out.reshape(rows_local, block, parts, cols_local, LANES)
    return out.transpose(0, 1, 3, 2, 4).reshape(rows_local, block, cols_local, width)


def solution(mesh):
    in_specs = (
        P(None, "row", None, "col"),
        P("row", None, None),
        P("row", None, None),
        P(),
        P(),
        P(),
    )
    out_specs = P(None, "row", None, "col")
    body = functools.partial(shards, mesh.shape["row"], mesh.shape["col"])
    return jax.shard_map(body, mesh=mesh, in_specs=in_specs, out_specs=out_specs, check_vma=False)
```

```python
import functools

import jax
import jax.numpy as jnp
from jax import lax
from jax.experimental import pallas as pl
from jax.experimental.pallas import tpu as pltpu
from jax.sharding import PartitionSpec as P


ANY = pl.BlockSpec(memory_space=pl.ANY)
SMEM = pl.BlockSpec(memory_space=pltpu.SMEM)
VMEM = pl.BlockSpec(memory_space=pltpu.VMEM)
LANES = 128


def in_hbm(x):
    return pltpu.with_memory_space_constraint(x, pltpu.HBM)


class Plan:
    def __init__(self, rows_n, cols_n, rows_local, cols_local, block, rank, blocks):
        self.rows_n, self.cols_n = rows_n, cols_n
        self.halves = rows_n // 2
        self.window = 2 * rows_local
        self.rows_local, self.cols_local = rows_local, cols_local
        self.row_cap = self.window // rows_n
        self.col_cap = self.window // cols_n
        self.half_cap = self.row_cap // 2
        self.block, self.rank, self.blocks = block, rank, blocks
        self.step = cols_local * (block // LANES)
        assert cols_n == 2 * rows_n and self.half_cap == self.col_cap

    def here(self):
        row, col = lax.axis_index("row"), lax.axis_index("col")
        return row, col, row // 2, row % 2

    def parity(self, group, col):
        return (col // self.rows_n + (col // self.halves) % 2 + 2 * group // self.halves) % 2

    def owns_diag(self, group, col):
        return (col % self.rows_n) // 2 == group


def read_map(plan, block_map, valid_rows, child, group, count, where=None):
    for slot in range(plan.window):
        count[slot] = 0
        if where is not None:
            where[slot] = 0
    for i in range(plan.blocks):
        spot = block_map[child, group * plan.blocks + i] - group * plan.window
        count[spot] = valid_rows[child, group * plan.blocks + i]
        if where is not None:
            where[spot] = i


def keep_rows(plan, x, count):
    pos = lax.broadcasted_iota(jnp.int32, (plan.block, 1), 0)
    return jnp.where(pos < count, x, jnp.zeros_like(x))


def project(x, mixer):
    dims = (((0,), (1,)), ((), ()))
    return lax.dot_general(mixer, x, dims, preferred_element_type=jnp.float32).astype(x.dtype)


def pack_rows_kernel(plan, block_map, valid_rows, generators, *refs):
    outs, (where, count, sems) = refs[:-3], refs[-3:]
    _, col, group, child = plan.here()
    read_map(plan, block_map, valid_rows, child, group, count, where)
    copies = []
    for i, out in enumerate(outs):
        d, k = 1 + i // 2, i % 2
        aim = (group + plan.halves - d) % plan.halves
        target = 2 * aim + (child + k) % 2
        parity = plan.parity(aim, col)
        for j in range(plan.half_cap):
            source = where[(2 * j + parity) * plan.rows_n + target]
            copies.append(pltpu.make_async_copy(
                generators.at[source], out.at[j], sems.at[len(copies)]))
            copies[-1].start()
    for copy in copies:
        copy.wait()


def pack_rest_kernel(plan, block_map, valid_rows, generators, diagonal, coupling, mine, *refs):
    outs, (where, count, picked, mixer, sems) = refs[:-5], refs[-5:]
    _, col, group, child = plan.here()
    read_map(plan, block_map, valid_rows, child, group, count, where)
    copies = []

    def go(source, target):
        copies.append(pltpu.make_async_copy(source, target, sems.at[len(copies)]))
        copies[-1].start()
        return copies[-1]

    first = [go(coupling.at[child], mixer)]
    for s in range(plan.col_cap):
        first.append(go(generators.at[where[s * plan.cols_n + col]], picked.at[s]))
    for s in range(plan.col_cap):
        go(diagonal.at[where[s * plan.cols_n + col]], mine.at[plan.row_cap + plan.col_cap + s])
    partner = 2 * group + (child + 1) % 2
    for q in range(plan.row_cap):
        go(generators.at[where[q * plan.rows_n + partner]], mine.at[q])
    for copy in first:
        copy.wait()
    for s in range(plan.col_cap):
        masked = keep_rows(plan, picked[s], count[s * plan.cols_n + col])
        mine[plan.row_cap + s] = project(masked, mixer[...])
    for copy in copies[len(first):]:
        copy.wait()
    for i, out in enumerate(outs):
        aim = (group + plan.halves - (i + 1)) % plan.halves
        owns = plan.owns_diag(aim, col)

        @pl.when(owns)
        def _():
            for s in range(plan.col_cap):
                out[s] = mine[plan.row_cap + plan.col_cap + s]

        @pl.when(jnp.logical_not(owns))
        def _():
            for s in range(plan.col_cap):
                out[s] = mine[plan.row_cap + s]


def project_kernel(plan, block_map, valid_rows, coupling, *refs):
    halves = plan.halves
    rows_in, (out, count, mixer, sem) = refs[:-4], refs[-4:]
    row, col, group, child = plan.here()
    copy = pltpu.make_async_copy(coupling, mixer, sem)
    copy.start()
    copy.wait()
    for d in range(1, halves):
        aim = (group + d) % halves
        parity = plan.parity(group, col)
        for k in range(2):
            who = (child + k) % 2
            read_map(plan, block_map, valid_rows, who, aim, count)
            for j in range(plan.half_cap):
                rows = count[(2 * j + parity) * plan.rows_n + row]
                masked = keep_rows(plan, rows_in[2 * (d - 1) + k][j], rows)
                out[d - 1, k, j] = project(masked, mixer[who])


def strided(plan, part, b):
    return pl.ds(part * plan.cols_local + b, plan.block, stride=plan.step)


def add_tile(plan, total, a, b, value):
    for part in range(plan.block // LANES):
        rows = strided(plan, part, b)
        total[a, rows, :] += value[:, part * LANES:(part + 1) * LANES]


def diag_tile(plan, pair, counts):
    x_pos = lax.broadcasted_iota(jnp.int32, (plan.block, 1), 0)
    y_pos = lax.broadcasted_iota(jnp.int32, (1, plan.block), 1)
    return sum(
        jnp.where((x_pos < n) & (y_pos < n), x.astype(jnp.float32), 0.0)
        for x, n in zip(pair, counts))


def matmul(x, y):
    return jnp.dot(x, y, preferred_element_type=jnp.float32)


def begin_kernel(plan, block_map, valid_rows, generators, diagonal, mine, theirs, front,
                 total, left, count_a, count_b, where, own_rows, own_diag, sems):
    row, col, group, child = plan.here()
    read_map(plan, block_map, valid_rows, child, group, count_a, where)
    read_map(plan, block_map, valid_rows, (child + 1) % 2, group, count_b)
    counts = (count_a, count_b)
    loads = []
    for q in range(plan.row_cap):
        loads.append(pltpu.make_async_copy(
            generators.at[where[q * plan.rows_n + row]], own_rows.at[q], sems.at[q]))
    for s in range(plan.col_cap):
        loads.append(pltpu.make_async_copy(
            diagonal.at[where[s * plan.cols_n + col]], own_diag.at[s],
            sems.at[plan.row_cap + s]))
    base = plan.row_cap + plan.col_cap
    reads = []
    for i in range(plan.rows_local):
        a = (group * plan.row_cap + i) % plan.rows_local
        reads.append(pltpu.make_async_copy(front.at[a], total.at[a], sems.at[base + i]))
    for copy in loads + reads:
        copy.start()
    for copy in loads:
        copy.wait()
    for q in range(plan.row_cap):
        where_q = q * plan.rows_n + row
        span = pl.ds(q * plan.block, plan.block)
        left[0, span, :] = keep_rows(plan, own_rows[q], count_a[where_q])
        left[1, span, :] = keep_rows(plan, theirs[q], count_b[where_q])
    for copy in reads[: plan.row_cap]:
        copy.wait()
    for s in range(plan.col_cap):
        value = matmul(left[0], mine[plan.row_cap + s]) + matmul(left[1], theirs[plan.row_cap + s])
        b = group * plan.col_cap + s
        for q in range(plan.row_cap):
            a = group * plan.row_cap + q
            add_tile(plan, total, a, b, value[q * plan.block:(q + 1) * plan.block])

    @pl.when(row == col % plan.rows_n)
    def _():
        for s in range(plan.col_cap):
            a = group * plan.row_cap + 2 * s + col // plan.rows_n
            b = group * plan.col_cap + s
            n = [count[s * plan.cols_n + col] for count in counts]
            pair = (own_diag[s], theirs[plan.row_cap + plan.col_cap + s])
            add_tile(plan, total, a, b, diag_tile(plan, pair, n))

    for copy in reads[plan.row_cap:]:
        copy.wait()


def finish_kernel(plan, block_map, valid_rows, left, mine, theirs, formed, formed_too, *refs):
    halves = plan.halves
    groups = [refs[6 * i: 6 * i + 6] for i in range(halves - 1)]
    _, out, total, count_a, count_b, far, right, sems = refs[6 * (halves - 1):]
    row, col, group, child = plan.here()
    owns = plan.owns_diag(group, col)
    main = row == col % plan.rows_n
    half = plan.half_cap

    for e in range(1, halves):
        direct, swapped = groups[e - 1][4:]
        for k in range(2):
            @pl.when(main)
            def _():
                for s in range(plan.col_cap):
                    right[e - 1, k, s] = formed[e - 1, k, s]

            @pl.when(owns & jnp.logical_not(main))
            def _():
                for s in range(plan.col_cap):
                    right[e - 1, k, s] = formed_too[e - 1, 1 - k, s]

            @pl.when(jnp.logical_not(owns))
            def _():
                for s in range(plan.col_cap):
                    right[e - 1, k, s] = (direct, swapped)[k][s]

    writes = []

    def write(a):
        writes.append(pltpu.make_async_copy(total.at[a], out.at[a], sems.at[len(writes)]))
        writes[-1].start()

    def rights(e, k, s):
        if e > 0:
            return right[e - 1, k, s]
        return (mine, theirs)[k][plan.row_cap + s]

    for g in range(2):
        span = pl.ds(g * half * plan.block, half * plan.block)
        for e in range(1, halves):
            for s in range(plan.col_cap):
                value = matmul(left[0, span, :], rights(e, 0, s))
                value += matmul(left[1, span, :], rights(e, 1, s))
                b = (group + e) % halves * plan.col_cap + s
                for j in range(half):
                    a = group * plan.row_cap + g * half + j
                    add_tile(plan, total, a, b, value[j * plan.block:(j + 1) * plan.block])
        for j in range(half):
            write(group * plan.row_cap + g * half + j)

    for d in range(1, halves):
        aim = (group + d) % halves
        read_map(plan, block_map, valid_rows, child, aim, count_a)
        read_map(plan, block_map, valid_rows, (child + 1) % 2, aim, count_b)
        counts = (count_a, count_b)
        parity = plan.parity(group, col)
        for g in range(2):
            odd = (parity + g) % 2
            for k in range(2):
                for j in range(half):
                    rows = counts[k][(2 * j + odd) * plan.rows_n + row]
                    far[k, pl.ds(j * plan.block, plan.block), :] = keep_rows(
                        plan, groups[d - 1][2 * g + k][j], rows)
            for e in range(halves):
                for s in range(plan.col_cap):
                    value = matmul(far[0], rights(e, 0, s)) + matmul(far[1], rights(e, 1, s))
                    b = (group + e) % halves * plan.col_cap + s
                    for j in range(half):
                        a = aim * plan.row_cap + 2 * j + odd
                        add_tile(plan, total, a, b, value[j * plan.block:(j + 1) * plan.block])
            if g == 0:
                @pl.when(main)
                def _():
                    for s in range(plan.col_cap):
                        a = aim * plan.row_cap + 2 * s + odd
                        b = aim * plan.col_cap + s
                        n = [count[s * plan.cols_n + col] for count in counts]
                        pair = (groups[d - 1][4][s], groups[d - 1][5][s])
                        add_tile(plan, total, a, b, diag_tile(plan, pair, n))
            for j in range(half):
                write(aim * plan.row_cap + 2 * j + odd)
    for copy in writes:
        copy.wait()


def shards(rows_n, cols_n, parent_front, generators, diagonal_blocks, coupling, block_map, valid_rows):
    rows_local, block, cols_local, width = parent_front.shape
    blocks, _, rank = generators.shape
    plan = Plan(rows_n, cols_n, rows_local, cols_local, block, rank, blocks)
    halves, row_cap, col_cap, half = plan.halves, plan.row_cap, plan.col_cap, plan.half_cap
    dt = generators.dtype
    parts = width // LANES
    table = pltpu.SMEM((plan.window,), jnp.int32)

    def shape(*lead):
        return jax.ShapeDtypeStruct(lead + (block, rank), dt)

    def sems(n):
        return pltpu.SemaphoreType.DMA((n,))

    def call(kernel, out_shape, in_specs, out_specs, scratch, mib, args, aliases={}):
        return pl.pallas_call(
            functools.partial(kernel, plan), out_shape=out_shape, in_specs=in_specs,
            out_specs=out_specs, scratch_shapes=scratch,
            input_output_aliases=aliases,
            compiler_params=pltpu.CompilerParams(vmem_limit_bytes=mib << 20))(*args)

    front = parent_front.reshape(rows_local, block, cols_local, parts, LANES)
    front = front.transpose(0, 1, 3, 2, 4).reshape(rows_local, block * plan.step, LANES)
    block_map, valid_rows, generators, diagonal_blocks, coupling, front = map(
        in_hbm, (block_map, valid_rows, generators, diagonal_blocks, coupling, front))

    def send(x, move):
        pairs = [
            (row * cols_n + col, to_row * cols_n + to_col)
            for row in range(rows_n)
            for col in range(cols_n)
            for to_row, to_col in [move(row, col)]
        ]
        return lax.ppermute(x, ("row", "col"), pairs)

    def across(d, k):
        return lambda row, col: (2 * ((row // 2 - d) % halves) + (row % 2 + k) % 2, col)

    def partner(row, col):
        return row ^ 1, col

    def pair(row, col):
        return row, col ^ halves

    flows = [(d, k) for d in range(1, halves) for k in range(2)]
    rows_out = call(
        pack_rows_kernel, [shape(half)] * len(flows), [SMEM, SMEM, ANY],
        [VMEM] * len(flows), [table, table, sems(len(flows) * half)], 8,
        (block_map, valid_rows, generators))
    near = {flow: send(x, across(*flow)) for flow, x in zip(flows, rows_out)}
    mine, *cols_out = call(
        pack_rest_kernel, [shape(row_cap + 2 * col_cap)] + [shape(col_cap)] * (halves - 1),
        [SMEM, SMEM, ANY, ANY, ANY], [VMEM] * halves,
        [table, table, pltpu.VMEM((col_cap, block, rank), dt), pltpu.VMEM((rank, rank), dt),
         sems(1 + 2 * col_cap + row_cap)], 12,
        (block_map, valid_rows, generators, diagonal_blocks, coupling))
    direct = {d: send(cols_out[d - 1], across(d, 0)) for d in range(1, halves)}
    theirs = send(mine, partner)
    total, left = call(
        begin_kernel,
        [jax.ShapeDtypeStruct(front.shape, front.dtype),
         jax.ShapeDtypeStruct((2, row_cap * block, rank), dt)],
        [SMEM, SMEM, ANY, ANY, VMEM, VMEM, ANY], [VMEM] * 2,
        [table, table, table, pltpu.VMEM((row_cap, block, rank), dt),
         pltpu.VMEM((col_cap, block, block), dt), sems(row_cap + col_cap + rows_local)], 24,
        (block_map, valid_rows, generators, diagonal_blocks, mine, theirs, front))
    passed = {flow: send(near[flow], pair) for flow in flows}
    formed = call(
        project_kernel, shape(halves - 1, 2, col_cap),
        [SMEM, SMEM, ANY] + [VMEM] * len(flows), VMEM,
        [table, pltpu.VMEM((2, rank, rank), dt), pltpu.SemaphoreType.DMA], 12,
        (block_map, valid_rows, coupling, *(near[flow] for flow in flows)))
    formed_too = send(formed, partner)
    swapped = {d: send(direct[d], partner) for d in range(1, halves)}
    rest = []
    for d in range(1, halves):
        rest += [near[d, 0], near[d, 1], passed[d, 0], passed[d, 1], direct[d], swapped[d]]
    args = (block_map, valid_rows, left, mine, theirs, formed, formed_too, *rest, total)
    out, _ = call(
        finish_kernel, [jax.ShapeDtypeStruct(front.shape, front.dtype)] * 2,
        [SMEM, SMEM] + [VMEM] * (len(args) - 2), [ANY, VMEM],
        [table, table, pltpu.VMEM((2, half * block, rank), dt),
         pltpu.VMEM((halves - 1, 2, col_cap, block, rank), dt), sems(rows_local)],
        24, args, {len(args) - 1: 1})
    out = out.reshape(rows_local, block, parts, cols_local, LANES)
    return out.transpose(0, 1, 3, 2, 4).reshape(rows_local, block, cols_local, width)


def solution(mesh):
    in_specs = (
        P(None, "row", None, "col"),
        P("row", None, None),
        P("row", None, None),
        P(),
        P(),
        P(),
    )
    out_specs = P(None, "row", None, "col")

    def body(*args):
        return shards(mesh.shape["row"], mesh.shape["col"], *args)

    return jax.shard_map(body, mesh=mesh, in_specs=in_specs, out_specs=out_specs, check_vma=False)
```

```python
import functools

import jax
import jax.numpy as jnp
from jax import lax
from jax.experimental import pallas as pl
from jax.experimental.pallas import tpu as pltpu
from jax.sharding import PartitionSpec as P


ANY = pl.BlockSpec(memory_space=pl.ANY)
SMEM = pl.BlockSpec(memory_space=pltpu.SMEM)
VMEM = pl.BlockSpec(memory_space=pltpu.VMEM)
LANES = 128


def in_hbm(x):
    return pltpu.with_memory_space_constraint(x, pltpu.HBM)


class Plan:
    def __init__(self, rows_n, cols_n, rows_local, cols_local, block, rank, blocks):
        self.rows_n, self.cols_n = rows_n, cols_n
        self.halves = rows_n // 2
        self.window = 2 * rows_local
        self.rows_local, self.cols_local = rows_local, cols_local
        self.row_cap = self.window // rows_n
        self.col_cap = self.window // cols_n
        self.half_cap = self.row_cap // 2
        self.unit = self.half_cap * block // 2
        self.block, self.rank, self.blocks = block, rank, blocks
        self.step = cols_local * (block // LANES)
        assert cols_n == 2 * rows_n and self.half_cap == self.col_cap

    def here(self):
        row, col = lax.axis_index("row"), lax.axis_index("col")
        return row, col, row // 2, row % 2

    def parity(self, group, col):
        return (col // self.rows_n + (col // self.halves) % 2 + 2 * group // self.halves) % 2

    def owns_diag(self, group, col):
        return (col % self.rows_n) // 2 == group


def read_map(plan, block_map, valid_rows, child, group, count, where=None):
    for slot in range(plan.window):
        count[slot] = 0
        if where is not None:
            where[slot] = 0
    for i in range(plan.blocks):
        spot = block_map[child, group * plan.blocks + i] - group * plan.window
        count[spot] = valid_rows[child, group * plan.blocks + i]
        if where is not None:
            where[spot] = i


def keep_rows(x, count, start=0):
    pos = lax.broadcasted_iota(jnp.int32, (x.shape[0], 1), 0) + start
    return jnp.where(pos < count, x, jnp.zeros_like(x))


def keep_both(x, count):
    pos = lax.broadcasted_iota(jnp.int32, (1, x.shape[1]), 1)
    return jnp.where(pos < count, keep_rows(x, count), jnp.zeros_like(x))


def matmul(x, y):
    return jnp.dot(x, y, preferred_element_type=jnp.float32)


def project(x, mixer):
    dims = (((0,), (1,)), ((), ()))
    return lax.dot_general(mixer, x, dims, preferred_element_type=jnp.float32).astype(x.dtype)


def pack_rows_kernel(plan, block_map, valid_rows, generators, *refs):
    outs, (map_s, valid_s, every, where, count, sems) = refs[:-6], refs[-6:]
    _, col, group, child = plan.here()
    copies = [
        pltpu.make_async_copy(source, target, sems.at[i])
        for i, (source, target) in enumerate(
            ((generators, every), (block_map, map_s), (valid_rows, valid_s)))
    ]
    for copy in copies:
        copy.start()
    copies[1].wait()
    copies[2].wait()
    read_map(plan, map_s, valid_s, child, group, count, where)
    copies[0].wait()
    whole = plan.unit // plan.block
    side = col % 2
    for i, out in enumerate(outs):
        d, k = 1 + i // 2, i % 2
        aim = (group + plan.halves - d) % plan.halves
        target = 2 * aim + (child + k) % 2
        parity = plan.parity(aim, col)
        for j in range(max(whole, 1)):
            slot = (2 * (side * whole + j) + parity) * plan.rows_n + target
            if whole:
                out[pl.ds(j * plan.block, plan.block), :] = keep_rows(every[where[slot]], count[slot])
            else:
                start = pl.multiple_of(side * plan.unit, plan.unit)
                part = every[where[slot], pl.ds(start, plan.unit), :]
                out[...] = keep_rows(part, count[slot], start)


def pack_rest_kernel(plan, block_map, valid_rows, generators, diagonal, coupling, mine, own, *refs):
    outs, (where, count, picked, mixer, sems) = refs[:-5], refs[-5:]
    row, col, group, child = plan.here()
    read_map(plan, block_map, valid_rows, child, group, count, where)
    copies = []

    def go(source, target):
        copies.append(pltpu.make_async_copy(source, target, sems.at[len(copies)]))
        copies[-1].start()

    cols = [s * plan.cols_n + col for s in range(plan.col_cap)]
    mates = [q * plan.rows_n + 2 * group + (child + 1) % 2 for q in range(plan.row_cap)]
    selves = [q * plan.rows_n + row for q in range(plan.row_cap)]
    diags = plan.row_cap + plan.col_cap
    go(coupling.at[child], mixer)
    for s in range(plan.col_cap):
        go(generators.at[where[cols[s]]], picked.at[s])
    for s in range(plan.col_cap):
        go(diagonal.at[where[cols[s]]], mine.at[diags + s])
    for q in range(plan.row_cap):
        go(generators.at[where[mates[q]]], mine.at[q])
    for q in range(plan.row_cap):
        go(generators.at[where[selves[q]]], own.at[q])
    for copy in copies:
        copy.wait()
    for s in range(plan.col_cap):
        mine[plan.row_cap + s] = project(keep_rows(picked[s], count[cols[s]]), mixer[...])
        mine[diags + s] = keep_both(mine[diags + s], count[cols[s]])
    for q in range(plan.row_cap):
        mine[q] = keep_rows(mine[q], count[mates[q]])
        own[q] = keep_rows(own[q], count[selves[q]])
    for i, out in enumerate(outs):
        aim = (group + plan.halves - (i + 1)) % plan.halves
        owns = plan.owns_diag(aim, col)

        @pl.when(owns)
        def _():
            for s in range(plan.col_cap):
                out[s] = mine[diags + s]

        @pl.when(jnp.logical_not(owns))
        def _():
            for s in range(plan.col_cap):
                out[s] = mine[plan.row_cap + s]


def join(plan, target, k, here, there, side):
    first = pl.multiple_of(side * plan.unit, plan.unit)
    second = pl.multiple_of((1 - side) * plan.unit, plan.unit)
    target[k, pl.ds(first, plan.unit), :] = here[...]
    target[k, pl.ds(second, plan.unit), :] = there[...]


def project_kernel(plan, coupling, *refs):
    n = 4 * (plan.halves - 1)
    parts, formed, fars = refs[:n], refs[n], refs[n + 1:]
    _, col, _, child = plan.here()
    for d in range(1, plan.halves):
        for k in range(2):
            here, there = parts[4 * (d - 1) + 2 * k: 4 * (d - 1) + 2 * k + 2]
            join(plan, fars[d - 1], k, here, there, col % 2)
            mixer = coupling[(child + k) % 2]
            for j in range(plan.half_cap):
                rows = fars[d - 1][k, pl.ds(j * plan.block, plan.block), :]
                formed[d - 1, k, j] = project(rows, mixer)


def add_tile(plan, total, a, b, value):
    for part in range(plan.block // LANES):
        rows = pl.ds(part * plan.cols_local + b, plan.block, stride=plan.step)
        total[a, rows, :] += value[:, part * LANES:(part + 1) * LANES]


def add_tiles(plan, total, steps, b, value):
    for j, a in enumerate(steps):
        add_tile(plan, total, a, b, value[j * plan.block:(j + 1) * plan.block])


def begin_kernel(plan, own, mine, theirs, front, total, sems):
    row, col, group, _ = plan.here()
    reads = []
    for i in range(plan.rows_local):
        a = (group * plan.row_cap + i) % plan.rows_local
        reads.append(pltpu.make_async_copy(front.at[a], total.at[a], sems.at[i]))
        reads[-1].start()
    for copy in reads[: plan.row_cap]:
        copy.wait()
    rows = plan.row_cap * plan.block
    steps = [group * plan.row_cap + q for q in range(plan.row_cap)]
    left = [own[...].reshape(rows, plan.rank),
            theirs[pl.ds(0, plan.row_cap)].reshape(rows, plan.rank)]
    for s in range(plan.col_cap):
        value = matmul(left[0], mine[plan.row_cap + s]) + matmul(left[1], theirs[plan.row_cap + s])
        add_tiles(plan, total, steps, group * plan.col_cap + s, value)

    @pl.when(row == col % plan.rows_n)
    def _():
        for s in range(plan.col_cap):
            a = group * plan.row_cap + 2 * s + col // plan.rows_n
            slot = plan.row_cap + plan.col_cap + s
            value = mine[slot].astype(jnp.float32) + theirs[slot].astype(jnp.float32)
            add_tile(plan, total, a, group * plan.col_cap + s, value)

    for copy in reads[plan.row_cap:]:
        copy.wait()


def write_out(total, out, steps, sems, copies):
    for a in steps:
        copies.append(pltpu.make_async_copy(total.at[a], out.at[a], sems.at[len(copies)]))
        copies[-1].start()


def middle_kernel(plan, own, mine, theirs, formed, formed_too, *refs):
    halves, half = plan.halves, plan.half_cap
    groups = [refs[3 * i: 3 * i + 3] for i in range(halves - 1)]
    _, out, total, right, sems = refs[3 * (halves - 1):]
    row, col, group, _ = plan.here()
    owns = plan.owns_diag(group, col)
    main = row == col % plan.rows_n

    def choose(pick):
        for e in range(1, halves):
            for k in range(2):
                for s in range(plan.col_cap):
                    right[e, k, s] = pick(e, k, s)

    @pl.when(main)
    def _():
        choose(lambda e, k, s: formed[e - 1, k, s])

    @pl.when(owns & jnp.logical_not(main))
    def _():
        choose(lambda e, k, s: formed_too[e - 1, 1 - k, s])

    @pl.when(jnp.logical_not(owns))
    def _():
        choose(lambda e, k, s: groups[e - 1][k][s])

    for s in range(plan.col_cap):
        right[0, 0, s] = mine[plan.row_cap + s]
        right[0, 1, s] = theirs[plan.row_cap + s]
    copies = []
    rows = half * plan.block
    for g in range(2):
        steps = [group * plan.row_cap + g * half + j for j in range(half)]
        left = [own[pl.ds(g * half, half)].reshape(rows, plan.rank),
                theirs[pl.ds(g * half, half)].reshape(rows, plan.rank)]
        for e in range(1, halves):
            for s in range(plan.col_cap):
                value = matmul(left[0], right[e, 0, s]) + matmul(left[1], right[e, 1, s])
                add_tiles(plan, total, steps, (group + e) % halves * plan.col_cap + s, value)
        write_out(total, out, steps, sems, copies)
    parity = plan.parity(group, col)
    for d in range(1, halves):
        direct, swapped, far = groups[d - 1]
        aim = (group + d) % halves
        steps = [aim * plan.row_cap + 2 * j + parity for j in range(half)]

        @pl.when(main)
        def _():
            for s in range(plan.col_cap):
                value = direct[s].astype(jnp.float32) + swapped[s].astype(jnp.float32)
                add_tile(plan, total, steps[s], aim * plan.col_cap + s, value)

        for e in range(halves):
            for s in range(plan.col_cap):
                value = matmul(far[0], right[e, 0, s]) + matmul(far[1], right[e, 1, s])
                add_tiles(plan, total, steps, (group + e) % halves * plan.col_cap + s, value)
        write_out(total, out, steps, sems, copies)
    for copy in copies:
        copy.wait()


def last_kernel(plan, right, *refs):
    halves, half = plan.halves, plan.half_cap
    n = 4 * (halves - 1)
    parts, (total_in, out_in, out, total, far, sems) = refs[:n], refs[n:]
    _, col, group, _ = plan.here()
    odd = 1 - plan.parity(group, col)
    copies = []
    for d in range(1, halves):
        aim = (group + d) % halves
        steps = [aim * plan.row_cap + 2 * j + odd for j in range(half)]
        for k in range(2):
            here, there = parts[4 * (d - 1) + 2 * k: 4 * (d - 1) + 2 * k + 2]
            join(plan, far, k, here, there, col % 2)
        for e in range(halves):
            for s in range(plan.col_cap):
                value = matmul(far[0], right[e, 0, s]) + matmul(far[1], right[e, 1, s])
                add_tiles(plan, total, steps, (group + e) % halves * plan.col_cap + s, value)
        write_out(total, out, steps, sems, copies)
    for copy in copies:
        copy.wait()


def shards(rows_n, cols_n, parent_front, generators, diagonal_blocks, coupling, block_map, valid_rows):
    rows_local, block, cols_local, width = parent_front.shape
    blocks, _, rank = generators.shape
    plan = Plan(rows_n, cols_n, rows_local, cols_local, block, rank, blocks)
    halves, row_cap, col_cap, half = plan.halves, plan.row_cap, plan.col_cap, plan.half_cap
    dt = generators.dtype
    parts = width // LANES
    table = pltpu.SMEM((plan.window,), jnp.int32)
    turns = range(1, halves)

    def shape(*lead):
        return jax.ShapeDtypeStruct(lead + (block, rank), dt)

    unit = jax.ShapeDtypeStruct((plan.unit, rank), dt)
    joined = jax.ShapeDtypeStruct((2, half * block, rank), dt)

    def sems(n):
        return pltpu.SemaphoreType.DMA((n,))

    def call(kernel, out_shape, in_specs, out_specs, scratch, mib, args, aliases={}):
        return pl.pallas_call(
            functools.partial(kernel, plan), out_shape=out_shape, in_specs=in_specs,
            out_specs=out_specs, scratch_shapes=scratch,
            input_output_aliases=aliases,
            compiler_params=pltpu.CompilerParams(vmem_limit_bytes=mib << 20))(*args)

    front = parent_front.reshape(rows_local, block, cols_local, parts, LANES)
    front = front.transpose(0, 1, 3, 2, 4).reshape(rows_local, block * plan.step, LANES)
    mixers = coupling
    block_map, valid_rows, generators, diagonal_blocks, coupling, front = map(
        in_hbm, (block_map, valid_rows, generators, diagonal_blocks, coupling, front))

    def send(x, move):
        pairs = [
            (row * cols_n + col, to_row * cols_n + to_col)
            for row in range(rows_n)
            for col in range(cols_n)
            for to_row, to_col in [move(row, col)]
        ]
        return lax.ppermute(x, ("row", "col"), pairs)

    def across(d, k):
        return lambda row, col: (2 * ((row // 2 - d) % halves) + (row % 2 + k) % 2, col)

    def partner(row, col):
        return row ^ 1, col

    def beside(row, col):
        return row, col ^ 1

    def along(row, col):
        return row, col ^ halves

    flows = [(d, k) for d in turns for k in range(2)]
    rows_out = call(
        pack_rows_kernel, [unit] * len(flows), [ANY] * 3,
        [VMEM] * len(flows),
        [pltpu.SMEM(block_map.shape, jnp.int32), pltpu.SMEM(block_map.shape, jnp.int32),
         pltpu.VMEM(generators.shape, dt), table, table, sems(3)], 8,
        (block_map, valid_rows, generators))
    near, beside_, along_, far_ = {}, {}, {}, {}
    for (d, k), x in zip(flows, rows_out):
        near[d, k] = send(x, across(d, k))
    mine, own, *cols_out = call(
        pack_rest_kernel,
        [shape(row_cap + 2 * col_cap), shape(row_cap)] + [shape(col_cap)] * (halves - 1),
        [SMEM, SMEM, ANY, ANY, ANY], [VMEM] * (halves + 1),
        [table, table, pltpu.VMEM((col_cap, block, rank), dt), pltpu.VMEM((rank, rank), dt),
         sems(1 + 2 * col_cap + 2 * row_cap)], 12,
        (block_map, valid_rows, generators, diagonal_blocks, coupling))
    direct = {d: send(cols_out[d - 1], across(d, 0)) for d in turns}
    theirs = send(mine, partner)
    for d, k in flows:
        beside_[d, k] = send(near[d, k], beside)
        along_[d, k] = send(near[d, k], along)
    total = call(
        begin_kernel, jax.ShapeDtypeStruct(front.shape, front.dtype),
        [VMEM] * 3 + [ANY], VMEM, [sems(rows_local)], 24, (own, mine, theirs, front))
    for d in turns:
        far_[d, 0] = send(beside_[d, 0], along)
        far_[d, 1] = send(along_[d, 1], beside)
    args = (mixers,) + tuple(x[flow] for flow in flows for x in (near, beside_))
    formed, *fars = call(
        project_kernel, [shape(halves - 1, 2, col_cap)] + [joined] * (halves - 1),
        [VMEM] * len(args), [VMEM] * halves, [], 12, args)
    formed_too = send(formed, partner)
    swapped = {d: send(direct[d], partner) for d in turns}
    args = (own, mine, theirs, formed, formed_too) + tuple(
        x for d in turns for x in (direct[d], swapped[d], fars[d - 1])) + (total,)
    whole = jax.ShapeDtypeStruct(front.shape, front.dtype)
    out, total, right = call(
        middle_kernel, [whole, whole, shape(halves, 2, col_cap)],
        [VMEM] * len(args), [ANY, VMEM, VMEM], [sems(rows_local)],
        24, args, {len(args) - 1: 1})
    args = (right,) + tuple(x[flow] for flow in flows for x in (along_, far_)) + (total, out)
    out, _ = call(
        last_kernel, [whole] * 2, [VMEM] * (len(args) - 1) + [ANY], [ANY, VMEM],
        [pltpu.VMEM(joined.shape, dt), sems(rows_local)],
        24, args, {len(args) - 1: 0, len(args) - 2: 1})
    out = out.reshape(rows_local, block, parts, cols_local, LANES)
    return out.transpose(0, 1, 3, 2, 4).reshape(rows_local, block, cols_local, width)


def solution(mesh):
    in_specs = (
        P(None, "row", None, "col"),
        P("row", None, None),
        P("row", None, None),
        P(),
        P(),
        P(),
    )
    out_specs = P(None, "row", None, "col")

    def body(*args):
        return shards(mesh.shape["row"], mesh.shape["col"], *args)

    return jax.shard_map(body, mesh=mesh, in_specs=in_specs, out_specs=out_specs, check_vma=False)
```

```python
import functools

import jax
import jax.numpy as jnp
from jax import lax
from jax.experimental import pallas as pl
from jax.experimental.pallas import tpu as pltpu
from jax.sharding import PartitionSpec as P


ANY = pl.BlockSpec(memory_space=pl.ANY)
SMEM = pl.BlockSpec(memory_space=pltpu.SMEM)
VMEM = pl.BlockSpec(memory_space=pltpu.VMEM)
LANES = 128
PIECES = 4


def in_hbm(x):
    return pltpu.with_memory_space_constraint(x, pltpu.HBM)


class Plan:
    def __init__(self, rows_n, cols_n, rows_local, cols_local, block, rank, blocks):
        self.rows_n, self.cols_n = rows_n, cols_n
        self.halves = rows_n // 2
        self.window = 2 * rows_local
        self.rows_local, self.cols_local = rows_local, cols_local
        self.row_cap = self.window // rows_n
        self.col_cap = self.window // cols_n
        self.half_cap = self.row_cap // 2
        self.unit = self.half_cap * block // 2
        self.block, self.rank, self.blocks = block, rank, blocks
        self.step = cols_local * (block // LANES)
        assert cols_n == 2 * rows_n and self.half_cap == self.col_cap

    def here(self):
        row, col = lax.axis_index("row"), lax.axis_index("col")
        return row, col, row // 2, row % 2

    def parity(self, group, col):
        return (col // self.rows_n + (col // self.halves) % 2 + 2 * group // self.halves) % 2

    def owns_diag(self, group, col):
        return (col % self.rows_n) // 2 == group


def read_map(plan, block_map, valid_rows, child, group, count, where=None):
    for slot in range(plan.window):
        count[slot] = 0
        if where is not None:
            where[slot] = 0
    for i in range(plan.blocks):
        spot = block_map[child, group * plan.blocks + i] - group * plan.window
        count[spot] = valid_rows[child, group * plan.blocks + i]
        if where is not None:
            where[spot] = i


def keep_rows(x, count, start=0):
    pos = lax.broadcasted_iota(jnp.int32, (x.shape[0], 1), 0) + start
    return jnp.where(pos < count, x, jnp.zeros_like(x))


def keep_both(x, count):
    pos = lax.broadcasted_iota(jnp.int32, (1, x.shape[1]), 1)
    return jnp.where(pos < count, keep_rows(x, count), jnp.zeros_like(x))


def matmul(x, y):
    return jnp.dot(x, y, preferred_element_type=jnp.float32)


def project(x, mixer):
    dims = (((0,), (1,)), ((), ()))
    return lax.dot_general(mixer, x, dims, preferred_element_type=jnp.float32).astype(x.dtype)


def pack_rows_kernel(plan, block_map, valid_rows, generators, coupling, every, mixers, *refs):
    outs, (map_s, valid_s, where, count, sems) = refs[:-5], refs[-5:]
    _, col, group, child = plan.here()
    copies = [
        pltpu.make_async_copy(source, target, sems.at[i])
        for i, (source, target) in enumerate(
            ((generators, every), (block_map, map_s), (valid_rows, valid_s), (coupling, mixers)))
    ]
    for copy in copies:
        copy.start()
    copies[1].wait()
    copies[2].wait()
    read_map(plan, map_s, valid_s, child, group, count, where)
    copies[0].wait()
    whole = plan.unit // plan.block
    side = col % 2
    for i, out in enumerate(outs):
        d, k = 1 + i // 2, i % 2
        aim = (group + plan.halves - d) % plan.halves
        target = 2 * aim + (child + k) % 2
        parity = plan.parity(aim, col)
        for j in range(max(whole, 1)):
            slot = (2 * (side * whole + j) + parity) * plan.rows_n + target
            if whole:
                out[pl.ds(j * plan.block, plan.block), :] = keep_rows(every[where[slot]], count[slot])
            else:
                start = pl.multiple_of(side * plan.unit, plan.unit)
                part = every[where[slot], pl.ds(start, plan.unit), :]
                out[...] = keep_rows(part, count[slot], start)
    copies[3].wait()


def pack_rest_kernel(plan, block_map, valid_rows, every, mixers, diagonal, front,
                     mine, own, base, *refs):
    outs, (map_s, valid_s, where, count, sems) = refs[:-5], refs[-5:]
    row, col, group, child = plan.here()
    diags = plan.row_cap + plan.col_cap
    copies = [
        pltpu.make_async_copy(source, target, sems.at[i])
        for i, (source, target) in enumerate(
            ((block_map, map_s), (valid_rows, valid_s),
             (front.at[pl.ds(group * plan.row_cap, plan.row_cap)], base)))
    ]
    for copy in copies:
        copy.start()
    copies[0].wait()
    copies[1].wait()
    read_map(plan, map_s, valid_s, child, group, count, where)
    loads = []
    for s in range(plan.col_cap):
        source = diagonal.at[where[s * plan.cols_n + col]]
        loads.append(pltpu.make_async_copy(source, mine.at[diags + s], sems.at[3 + s]))
        loads[-1].start()
    for s in range(plan.col_cap):
        slot = s * plan.cols_n + col
        masked = keep_rows(every[where[slot]], count[slot])
        mine[plan.row_cap + s] = project(masked, mixers[child])
    for target, to in ((mine, 2 * group + (child + 1) % 2), (own, row)):
        for q in range(plan.row_cap):
            slot = q * plan.rows_n + to
            target[q] = keep_rows(every[where[slot]], count[slot])
    for s in range(plan.col_cap):
        loads[s].wait()
        mine[diags + s] = keep_both(mine[diags + s], count[s * plan.cols_n + col])
    for i, out in enumerate(outs):
        aim = (group + plan.halves - (i + 1)) % plan.halves
        owns = plan.owns_diag(aim, col)

        @pl.when(owns)
        def _():
            for s in range(plan.col_cap):
                out[s] = mine[diags + s]

        @pl.when(jnp.logical_not(owns))
        def _():
            for s in range(plan.col_cap):
                out[s] = mine[plan.row_cap + s]

    copies[2].wait()


def join(plan, target, k, here, there, side):
    first = pl.multiple_of(side * plan.unit, plan.unit)
    second = pl.multiple_of((1 - side) * plan.unit, plan.unit)
    target[k, pl.ds(first, plan.unit), :] = here[...]
    target[k, pl.ds(second, plan.unit), :] = there[...]


def project_kernel(plan, coupling, *refs):
    turns = plan.halves - 1
    directs, refs = refs[:turns], refs[turns:]
    parts, (formed, leave), fars = refs[: 4 * turns], refs[4 * turns: 4 * turns + 2], refs[4 * turns + 2:]
    row, col, _, child = plan.here()
    main = row == col % plan.rows_n
    for d in range(1, plan.halves):
        for k in range(2):
            here, there = parts[4 * (d - 1) + 2 * k: 4 * (d - 1) + 2 * k + 2]
            join(plan, fars[d - 1], k, here, there, col % 2)

    @pl.when(main)
    def _():
        for d in range(1, plan.halves):
            for k in range(2):
                mixer = coupling[(child + k) % 2]
                for j in range(plan.half_cap):
                    rows = fars[d - 1][k, pl.ds(j * plan.block, plan.block), :]
                    value = project(rows, mixer)
                    formed[d - 1, k, j] = value
                    leave[d - 1, k, j] = value

    @pl.when(jnp.logical_not(main))
    def _():
        for d in range(1, plan.halves):
            for j in range(plan.half_cap):
                leave[d - 1, 0, j] = directs[d - 1][j]


def put_across(plan, base, from_a, total, a, b, value):
    for part in range(plan.block // LANES):
        rows = pl.ds(part * plan.cols_local + b, plan.block, stride=plan.step)
        total[a, rows, :] = base[from_a, rows, :] + value[:, part * LANES:(part + 1) * LANES]


def put_tile(plan, base, total, a, b, value):
    put_across(plan, base, a, total, a, b, value)


def put_tiles(plan, base, total, steps, b, value):
    for j, a in enumerate(steps):
        put_tile(plan, base, total, a, b, value[j * plan.block:(j + 1) * plan.block])


def in_pieces(source, target, sems, copies):
    step = source.shape[0] // PIECES
    for i in range(PIECES):
        part = pl.ds(i * step, step)
        copies.append(pltpu.make_async_copy(source.at[part], target.at[part], sems.at[len(copies)]))
        copies[-1].start()


def begin_kernel(plan, own, mine, theirs, base, front, total, rest, sems):
    row, col, group, _ = plan.here()
    reads = []
    for i in range(plan.rows_local - plan.row_cap):
        a = (group * plan.row_cap + plan.row_cap + i) % plan.rows_local
        in_pieces(front.at[a], rest.at[i], sems, reads)
    rows = plan.row_cap * plan.block
    left = own[...].reshape(rows, plan.rank)
    right = theirs[pl.ds(0, plan.row_cap)].reshape(rows, plan.rank)
    for s in range(plan.col_cap):
        value = matmul(left, mine[plan.row_cap + s]) + matmul(right, theirs[plan.row_cap + s])
        put_tiles(plan, base, total, range(plan.row_cap), group * plan.col_cap + s, value)

    @pl.when(row == col % plan.rows_n)
    def _():
        for s in range(plan.col_cap):
            slot = plan.row_cap + plan.col_cap + s
            value = mine[slot].astype(jnp.float32) + theirs[slot].astype(jnp.float32)
            put_tile(plan, total, total, 2 * s + col // plan.rows_n, group * plan.col_cap + s, value)

    for copy in reads:
        copy.wait()


def even_kernel(plan, mine, theirs, *refs):
    fars, (rest, even) = refs[:-2], refs[-2:]
    half = plan.half_cap
    _, col, group, _ = plan.here()
    parity = plan.parity(group, col)
    for d in range(1, plan.halves):
        far = fars[d - 1]
        for s in range(plan.col_cap):
            value = matmul(far[0], mine[plan.row_cap + s]) + matmul(far[1], theirs[plan.row_cap + s])
            for j in range(half):
                put_across(plan, rest, (d - 1) * plan.row_cap + 2 * j + parity,
                           even, (d - 1) * half + j, group * plan.col_cap + s,
                           value[j * plan.block:(j + 1) * plan.block])


def spread(plan, left, right, base, total, steps, group):
    for e in range(1, plan.halves):
        for s in range(plan.col_cap):
            value = matmul(left(0), right[e, 0, s]) + matmul(left(1), right[e, 1, s])
            put_tiles(plan, base, total, steps, (group + e) % plan.halves * plan.col_cap + s, value)


def middle_kernel(plan, own, mine, theirs, formed, swapped, *refs):
    halves, half, turns = plan.halves, plan.half_cap, plan.halves - 1
    directs, fars = refs[:turns], refs[turns: 2 * turns]
    base, rest, _, _, out, near, even, right, sems = refs[2 * turns:]
    row, col, group, _ = plan.here()
    owns = plan.owns_diag(group, col)
    main = row == col % plan.rows_n

    def choose(pick):
        for e in range(1, halves):
            for k in range(2):
                for s in range(plan.col_cap):
                    right[e, k, s] = pick(e - 1, k, s)

    @pl.when(main)
    def _():
        choose(lambda e, k, s: formed[e, k, s])

    @pl.when(owns & jnp.logical_not(main))
    def _():
        choose(lambda e, k, s: swapped[e, 1 - k, s])

    @pl.when(jnp.logical_not(owns))
    def _():
        choose(lambda e, k, s: swapped[e, 0, s] if k else directs[e][s])

    for s in range(plan.col_cap):
        right[0, 0, s] = mine[plan.row_cap + s]
        right[0, 1, s] = theirs[plan.row_cap + s]
    rows = half * plan.block
    copies = []
    for g in range(2):
        def left(k):
            return (own, theirs)[k][pl.ds(g * half, half)].reshape(rows, plan.rank)

        spread(plan, left, right, base, near, [g * half + j for j in range(half)], group)
        for q in range(half if g == 0 else 0):
            in_pieces(near.at[q], out.at[group * plan.row_cap + q], sems, copies)
    parity = plan.parity(group, col)
    for d in range(1, halves):
        def left(k):
            return fars[d - 1][k]

        first = (d - 1) * plan.row_cap

        @pl.when(row >= 0)
        def _():
            for e in range(1, halves):
                for s in range(plan.col_cap):
                    value = matmul(left(0), right[e, 0, s]) + matmul(left(1), right[e, 1, s])
                    b = (group + e) % halves * plan.col_cap + s
                    for j in range(half):
                        put_across(plan, rest, first + 2 * j + parity, even, (d - 1) * half + j, b,
                                   value[j * plan.block:(j + 1) * plan.block])

        @pl.when(main)
        def _():
            for s in range(plan.col_cap):
                value = directs[d - 1][s].astype(jnp.float32) + swapped[d - 1, 0, s].astype(jnp.float32)
                b = (group + d) % halves * plan.col_cap + s
                put_tile(plan, even, even, (d - 1) * half + s, b, value)
    for copy in copies:
        copy.wait()


def last_kernel(plan, right, *refs):
    halves, half, turns = plan.halves, plan.half_cap, plan.halves - 1
    parts, (rest, near, even, out_in, out, odd, far, sems) = refs[: 4 * turns], refs[4 * turns:]
    _, col, group, _ = plan.here()
    parity = plan.parity(group, col)
    copies = []

    def write(source, a):
        in_pieces(source, out.at[a], sems, copies)

    for q in range(half, plan.row_cap):
        write(near.at[q], group * plan.row_cap + q)
    for d in range(1, halves):
        for j in range(half):
            a = (group + d) % halves * plan.row_cap + 2 * j + parity
            write(even.at[(d - 1) * half + j], a)
    for d in range(1, halves):
        for k in range(2):
            here, there = parts[4 * (d - 1) + 2 * k: 4 * (d - 1) + 2 * k + 2]
            join(plan, far, k, here, there, col % 2)
        for j in range(half):
            for e in range(halves):
                for s in range(plan.col_cap):
                    rows = pl.ds(j * plan.block, plan.block)
                    value = matmul(far[0, rows, :], right[e, 0, s])
                    value += matmul(far[1, rows, :], right[e, 1, s])
                    b = (group + e) % halves * plan.col_cap + s
                    put_across(plan, rest, (d - 1) * plan.row_cap + 2 * j + 1 - parity,
                               odd, (d - 1) * half + j, b, value)
            a = (group + d) % halves * plan.row_cap + 2 * j + 1 - parity
            write(odd.at[(d - 1) * half + j], a)
    for copy in copies:
        copy.wait()


def shards(rows_n, cols_n, parent_front, generators, diagonal_blocks, coupling, block_map, valid_rows):
    rows_local, block, cols_local, width = parent_front.shape
    blocks, _, rank = generators.shape
    plan = Plan(rows_n, cols_n, rows_local, cols_local, block, rank, blocks)
    halves, row_cap, col_cap, half = plan.halves, plan.row_cap, plan.col_cap, plan.half_cap
    dt = generators.dtype
    parts = width // LANES
    table = pltpu.SMEM((plan.window,), jnp.int32)
    turns = range(1, halves)

    def shape(*lead):
        return jax.ShapeDtypeStruct(lead + (block, rank), dt)

    unit = jax.ShapeDtypeStruct((plan.unit, rank), dt)
    joined = jax.ShapeDtypeStruct((2, half * block, rank), dt)

    def sems(n):
        return pltpu.SemaphoreType.DMA((n,))

    def call(kernel, out_shape, in_specs, out_specs, scratch, mib, args, aliases={}):
        return pl.pallas_call(
            functools.partial(kernel, plan), out_shape=out_shape, in_specs=in_specs,
            out_specs=out_specs, scratch_shapes=scratch,
            input_output_aliases=aliases,
            compiler_params=pltpu.CompilerParams(vmem_limit_bytes=mib << 20))(*args)

    front = parent_front.reshape(rows_local, block, cols_local, parts, LANES)
    front = front.transpose(0, 1, 3, 2, 4).reshape(rows_local, block * plan.step, LANES)
    block_map, valid_rows, generators, diagonal_blocks, coupling, front = map(
        in_hbm, (block_map, valid_rows, generators, diagonal_blocks, coupling, front))

    def strip(n):
        return jax.ShapeDtypeStruct((n,) + front.shape[1:], front.dtype)

    def send(x, move):
        pairs = [
            (row * cols_n + col, to_row * cols_n + to_col)
            for row in range(rows_n)
            for col in range(cols_n)
            for to_row, to_col in [move(row, col)]
        ]
        return lax.ppermute(x, ("row", "col"), pairs)

    def across(d, k):
        return lambda row, col: (2 * ((row // 2 - d) % halves) + (row % 2 + k) % 2, col)

    def partner(row, col):
        return row ^ 1, col

    def beside(row, col):
        return row, col ^ 1

    def along(row, col):
        return row, col ^ halves

    flows = [(d, k) for d in turns for k in range(2)]
    maps = [pltpu.SMEM(block_map.shape, jnp.int32)] * 2 + [table] * 2
    every, mixers, *rows_out = call(
        pack_rows_kernel, [shape(blocks), shape(2)] + [unit] * len(flows), [ANY] * 4,
        [VMEM] * (2 + len(flows)), maps + [sems(4)], 8,
        (block_map, valid_rows, generators, coupling))
    near, beside_, along_, far_ = {}, {}, {}, {}
    for (d, k), x in zip(flows, rows_out):
        near[d, k] = send(x, across(d, k))
    mine, own, base, *cols_out = call(
        pack_rest_kernel,
        [shape(row_cap + 2 * col_cap), shape(row_cap), strip(row_cap)] + [shape(col_cap)] * (halves - 1),
        [ANY, ANY, VMEM, VMEM, ANY, ANY], [VMEM] * (halves + 2), maps + [sems(3 + col_cap)], 12,
        (block_map, valid_rows, every, mixers, diagonal_blocks, front))
    direct = {d: send(cols_out[d - 1], across(d, 0)) for d in turns}
    theirs = send(mine, partner)
    for d, k in flows:
        beside_[d, k] = send(near[d, k], beside)
        along_[d, k] = send(near[d, k], along)
    for d in turns:
        far_[d, 0] = send(beside_[d, 0], along)
        far_[d, 1] = send(along_[d, 1], beside)
    others = rows_local - row_cap
    args = (own, mine, theirs, base, front)
    near_rows, rest = call(
        begin_kernel, [strip(row_cap), strip(others)],
        [VMEM] * 4 + [ANY], [VMEM] * 2, [sems(others * PIECES)], 12, args)
    args = (mixers,) + tuple(direct[d] for d in turns) + tuple(
        x[flow] for flow in flows for x in (near, beside_))
    formed, leave, *fars = call(
        project_kernel, [shape(halves - 1, 2, col_cap)] * 2 + [joined] * (halves - 1),
        [VMEM] * len(args), [VMEM] * (1 + halves), [], 12, args)
    swapped = send(leave, partner)
    args = (mine, theirs, *fars, rest)
    even = call(even_kernel, strip(others // 2), [VMEM] * len(args), VMEM, [], 12, args)
    args = (own, mine, theirs, formed, swapped, *(direct[d] for d in turns), *fars,
            base, rest, near_rows, even)
    n = len(args)
    out, near_rows, even, right = call(
        middle_kernel,
        [strip(rows_local), strip(row_cap), strip(others // 2), shape(halves, 2, col_cap)],
        [VMEM] * n, [ANY] + [VMEM] * 3, [sems(half * PIECES)], 12, args, {n - 2: 1, n - 1: 2})
    args = (right,) + tuple(x[flow] for flow in flows for x in (along_, far_)) + (
        rest, near_rows, even, out)
    out = call(
        last_kernel, strip(rows_local), [VMEM] * (len(args) - 1) + [ANY], ANY,
        [pltpu.VMEM((others // 2,) + front.shape[1:], front.dtype),
         pltpu.VMEM(joined.shape, dt), sems((others + half) * PIECES)], 16, args, {len(args) - 1: 0})
    out = out.reshape(rows_local, block, parts, cols_local, LANES)
    return out.transpose(0, 1, 3, 2, 4).reshape(rows_local, block, cols_local, width)


def solution(mesh):
    in_specs = (
        P(None, "row", None, "col"),
        P("row", None, None),
        P("row", None, None),
        P(),
        P(),
        P(),
    )
    out_specs = P(None, "row", None, "col")

    def body(*args):
        return shards(mesh.shape["row"], mesh.shape["col"], *args)

    return jax.shard_map(body, mesh=mesh, in_specs=in_specs, out_specs=out_specs, check_vma=False)
```

```python
import functools

import jax
import jax.numpy as jnp
from jax import lax
from jax.experimental import pallas as pl
from jax.experimental.pallas import tpu as pltpu
from jax.sharding import PartitionSpec as P


ANY = pl.BlockSpec(memory_space=pl.ANY)
SMEM = pl.BlockSpec(memory_space=pltpu.SMEM)
VMEM = pl.BlockSpec(memory_space=pltpu.VMEM)
LANES = 128
PIECES = 1


def in_hbm(x):
    return pltpu.with_memory_space_constraint(x, pltpu.HBM)


class Plan:
    def __init__(self, rows_n, cols_n, rows_local, cols_local, block, rank, blocks):
        self.rows_n, self.cols_n = rows_n, cols_n
        self.halves = rows_n // 2
        self.window = 2 * rows_local
        self.rows_local, self.cols_local = rows_local, cols_local
        self.row_cap = self.window // rows_n
        self.col_cap = self.window // cols_n
        self.half_cap = self.row_cap // 2
        self.unit = self.half_cap * block // 2
        self.block, self.rank, self.blocks = block, rank, blocks
        self.step = cols_local * (block // LANES)
        assert cols_n == 2 * rows_n and self.half_cap == self.col_cap

    def here(self):
        row, col = lax.axis_index("row"), lax.axis_index("col")
        return row, col, row // 2, row % 2

    def parity(self, group, col):
        return (col // self.rows_n + (col // self.halves) % 2 + 2 * group // self.halves) % 2

    def owns_diag(self, group, col):
        return (col % self.rows_n) // 2 == group


def read_map(plan, block_map, valid_rows, child, group, count, where=None):
    for slot in range(plan.window):
        count[slot] = 0
        if where is not None:
            where[slot] = 0
    for i in range(plan.blocks):
        spot = block_map[child, group * plan.blocks + i] - group * plan.window
        count[spot] = valid_rows[child, group * plan.blocks + i]
        if where is not None:
            where[spot] = i


def keep_rows(x, count, start=0):
    pos = lax.broadcasted_iota(jnp.int32, (x.shape[0], 1), 0) + start
    return jnp.where(pos < count, x, jnp.zeros_like(x))


def keep_both(x, count):
    pos = lax.broadcasted_iota(jnp.int32, (1, x.shape[1]), 1)
    return jnp.where(pos < count, keep_rows(x, count), jnp.zeros_like(x))


def matmul(x, y):
    return jnp.dot(x, y, preferred_element_type=jnp.float32)


def project(x, mixer):
    dims = (((0,), (1,)), ((), ()))
    return lax.dot_general(mixer, x, dims, preferred_element_type=jnp.float32).astype(x.dtype)


def fill_unit(plan, out, every, where, count, target, parity, side):
    whole = plan.unit // plan.block
    for j in range(max(whole, 1)):
        slot = (2 * (side * whole + j) + parity) * plan.rows_n + target
        if whole:
            out[pl.ds(j * plan.block, plan.block), :] = keep_rows(every[where[slot]], count[slot])
        else:
            start = pl.multiple_of(side * plan.unit, plan.unit)
            part = every[where[slot], pl.ds(start, plan.unit), :]
            out[...] = keep_rows(part, count[slot], start)


def pack_rows_kernel(plan, block_map, valid_rows, generators, coupling, every, mixers, *refs):
    outs, (map_s, valid_s, where, count, sems) = refs[:-5], refs[-5:]
    _, col, group, child = plan.here()
    copies = [
        pltpu.make_async_copy(source, target, sems.at[i])
        for i, (source, target) in enumerate(
            ((generators, every), (block_map, map_s), (valid_rows, valid_s), (coupling, mixers)))
    ]
    for copy in copies:
        copy.start()
    copies[1].wait()
    copies[2].wait()
    read_map(plan, map_s, valid_s, child, group, count, where)
    copies[0].wait()
    side = col % 2
    for i, out in enumerate(outs):
        d, k = 1 + i // 2, i % 2
        aim = (group + plan.halves - d) % plan.halves
        fill_unit(plan, out, every, where, count, 2 * aim + (child + k) % 2, plan.parity(aim, col), side)
    copies[3].wait()


def pack_rest_kernel(plan, block_map, valid_rows, every, mixers, diagonal, front,
                     mine, own, base, *refs):
    turns = plan.halves - 1
    far_outs, outs, (map_s, valid_s, where, count, sems) = refs[:turns], refs[turns:-5], refs[-5:]
    row, col, group, child = plan.here()
    diags = plan.row_cap + plan.col_cap
    copies = [
        pltpu.make_async_copy(source, target, sems.at[i])
        for i, (source, target) in enumerate(
            ((block_map, map_s), (valid_rows, valid_s),
             (front.at[pl.ds(group * plan.row_cap, plan.row_cap)], base)))
    ]
    for copy in copies:
        copy.start()
    copies[0].wait()
    copies[1].wait()
    read_map(plan, map_s, valid_s, child, group, count, where)
    loads = []
    for s in range(plan.col_cap):
        source = diagonal.at[where[s * plan.cols_n + col]]
        loads.append(pltpu.make_async_copy(source, mine.at[diags + s], sems.at[3 + s]))
        loads[-1].start()
    for s in range(plan.col_cap):
        slot = s * plan.cols_n + col
        masked = keep_rows(every[where[slot]], count[slot])
        mine[plan.row_cap + s] = project(masked, mixers[child])
    for target, to in ((mine, 2 * group + (child + 1) % 2), (own, row)):
        for q in range(plan.row_cap):
            slot = q * plan.rows_n + to
            target[q] = keep_rows(every[where[slot]], count[slot])
    for i, out in enumerate(far_outs):
        aim = (group + plan.halves - (i + 1)) % plan.halves
        fill_unit(plan, out, every, where, count, 2 * aim + (child + 1) % 2,
                  1 - plan.parity(aim, col), 1 - col % 2)
    for s in range(plan.col_cap):
        loads[s].wait()
        mine[diags + s] = keep_both(mine[diags + s], count[s * plan.cols_n + col])
    for i, out in enumerate(outs):
        aim = (group + plan.halves - (i + 1)) % plan.halves
        owns = plan.owns_diag(aim, col)

        @pl.when(owns)
        def _():
            for s in range(plan.col_cap):
                out[s] = mine[diags + s]

        @pl.when(jnp.logical_not(owns))
        def _():
            for s in range(plan.col_cap):
                out[s] = mine[plan.row_cap + s]

    copies[2].wait()


def join(plan, target, k, here, there, side):
    first = pl.multiple_of(side * plan.unit, plan.unit)
    second = pl.multiple_of((1 - side) * plan.unit, plan.unit)
    target[k, pl.ds(first, plan.unit), :] = here[...]
    target[k, pl.ds(second, plan.unit), :] = there[...]


def project_kernel(plan, coupling, *refs):
    turns = plan.halves - 1
    directs, refs = refs[:turns], refs[turns:]
    parts, (formed, leave), fars = refs[: 4 * turns], refs[4 * turns: 4 * turns + 2], refs[4 * turns + 2:]
    row, col, _, child = plan.here()
    main = row == col % plan.rows_n
    for d in range(1, plan.halves):
        for k in range(2):
            here, there = parts[4 * (d - 1) + 2 * k: 4 * (d - 1) + 2 * k + 2]
            join(plan, fars[d - 1], k, here, there, col % 2)

    @pl.when(main)
    def _():
        for d in range(1, plan.halves):
            for k in range(2):
                mixer = coupling[(child + k) % 2]
                for j in range(plan.half_cap):
                    rows = fars[d - 1][k, pl.ds(j * plan.block, plan.block), :]
                    value = project(rows, mixer)
                    formed[d - 1, k, j] = value
                    leave[d - 1, k, j] = value

    @pl.when(jnp.logical_not(main))
    def _():
        for d in range(1, plan.halves):
            for j in range(plan.half_cap):
                leave[d - 1, 0, j] = directs[d - 1][j]


def put_across(plan, base, from_a, total, a, b, value):
    for part in range(plan.block // LANES):
        rows = pl.ds(part * plan.cols_local + b, plan.block, stride=plan.step)
        total[a, rows, :] = base[from_a, rows, :] + value[:, part * LANES:(part + 1) * LANES]


def put_tile(plan, base, total, a, b, value):
    put_across(plan, base, a, total, a, b, value)


def put_tiles(plan, base, total, steps, b, value):
    for j, a in enumerate(steps):
        put_tile(plan, base, total, a, b, value[j * plan.block:(j + 1) * plan.block])


def in_pieces(source, target, sems, copies):
    step = source.shape[0] // PIECES
    for i in range(PIECES):
        part = pl.ds(i * step, step)
        copies.append(pltpu.make_async_copy(source.at[part], target.at[part], sems.at[len(copies)]))
        copies[-1].start()


def load_kernel(plan, front, rest, sems):
    _, _, group, _ = plan.here()
    reads = []
    for i in range(plan.rows_local - plan.row_cap):
        a = (group * plan.row_cap + plan.row_cap + i) % plan.rows_local
        in_pieces(front.at[a], rest.at[i], sems, reads)
    for copy in reads:
        copy.wait()


def begin_kernel(plan, own, mine, theirs, base, total):
    row, col, group, _ = plan.here()
    rows = plan.row_cap * plan.block
    left = own[...].reshape(rows, plan.rank)
    right = theirs[pl.ds(0, plan.row_cap)].reshape(rows, plan.rank)
    for s in range(plan.col_cap):
        value = matmul(left, mine[plan.row_cap + s]) + matmul(right, theirs[plan.row_cap + s])
        put_tiles(plan, base, total, range(plan.row_cap), group * plan.col_cap + s, value)

    @pl.when(row == col % plan.rows_n)
    def _():
        for s in range(plan.col_cap):
            slot = plan.row_cap + plan.col_cap + s
            value = mine[slot].astype(jnp.float32) + theirs[slot].astype(jnp.float32)
            put_tile(plan, total, total, 2 * s + col // plan.rows_n, group * plan.col_cap + s, value)


def even_kernel(plan, mine, theirs, *refs):
    fars, (rest, even) = refs[:-2], refs[-2:]
    half = plan.half_cap
    _, col, group, _ = plan.here()
    parity = plan.parity(group, col)
    for d in range(1, plan.halves):
        far = fars[d - 1]
        for s in range(plan.col_cap):
            value = matmul(far[0], mine[plan.row_cap + s]) + matmul(far[1], theirs[plan.row_cap + s])
            for j in range(half):
                put_across(plan, rest, (d - 1) * plan.row_cap + 2 * j + parity,
                           even, (d - 1) * half + j, group * plan.col_cap + s,
                           value[j * plan.block:(j + 1) * plan.block])


def finish_kernel(plan, own, mine, theirs, formed, swapped, *refs):
    halves, half, turns = plan.halves, plan.half_cap, plan.halves - 1
    directs, fars, parts = refs[:turns], refs[turns: 2 * turns], refs[2 * turns: 6 * turns]
    base, rest, _, _, out, near, even, odd, far, right, sems = refs[6 * turns:]
    row, col, group, _ = plan.here()
    owns = plan.owns_diag(group, col)
    main = row == col % plan.rows_n

    def choose(pick):
        for e in range(1, halves):
            for k in range(2):
                for s in range(plan.col_cap):
                    right[e, k, s] = pick(e - 1, k, s)

    @pl.when(main)
    def _():
        choose(lambda e, k, s: formed[e, k, s])

    @pl.when(owns & jnp.logical_not(main))
    def _():
        choose(lambda e, k, s: swapped[e, 1 - k, s])

    @pl.when(jnp.logical_not(owns))
    def _():
        choose(lambda e, k, s: swapped[e, 0, s] if k else directs[e][s])

    for s in range(plan.col_cap):
        right[0, 0, s] = mine[plan.row_cap + s]
        right[0, 1, s] = theirs[plan.row_cap + s]
    copies = []

    def write(source, a):
        in_pieces(source, out.at[a], sems, copies)

    def spread(left, start, source, sources, total, places, first):
        rows = pl.ds(start, len(places) * plan.block)
        for e in range(first, halves):
            for s in range(plan.col_cap):
                value = matmul(left(0, rows), right[e, 0, s]) + matmul(left(1, rows), right[e, 1, s])
                b = (group + e) % halves * plan.col_cap + s
                for j, (a, place) in enumerate(zip(sources, places)):
                    put_across(plan, source, a, total, place, b,
                               value[j * plan.block:(j + 1) * plan.block])

    for g in range(2):
        def left(k, rows):
            value = (own, theirs)[k][pl.ds(g * half, half)]
            return value.reshape(half * plan.block, plan.rank)

        steps = range(g * half, g * half + half)
        spread(left, 0, base, steps, near, steps, 1)
        for q in steps:
            write(near.at[q], group * plan.row_cap + q)
    parity = plan.parity(group, col)
    for d in range(1, halves):
        places = range((d - 1) * half, d * half)
        first = (d - 1) * plan.row_cap
        top = (group + d) % halves * plan.row_cap

        @pl.when(row >= 0)
        def _():
            spread(lambda k, rows: fars[d - 1][k], 0, rest,
                   [first + 2 * j + parity for j in range(half)], even, places, 1)

        @pl.when(main)
        def _():
            for s in range(plan.col_cap):
                value = directs[d - 1][s].astype(jnp.float32) + swapped[d - 1, 0, s].astype(jnp.float32)
                put_tile(plan, even, even, places[s], (group + d) % halves * plan.col_cap + s, value)

        for j in range(half):
            write(even.at[places[j]], top + 2 * j + parity)
        for k in range(2):
            here, there = parts[4 * (d - 1) + 2 * k: 4 * (d - 1) + 2 * k + 2]
            join(plan, far, k, here, there, col % 2)
        for j in range(half):
            spread(lambda k, rows: far[k, rows, :], j * plan.block, rest,
                   [first + 2 * j + 1 - parity], odd, [places[j]], 0)
            write(odd.at[places[j]], top + 2 * j + 1 - parity)
    for copy in copies:
        copy.wait()


def shards(rows_n, cols_n, parent_front, generators, diagonal_blocks, coupling, block_map, valid_rows):
    rows_local, block, cols_local, width = parent_front.shape
    blocks, _, rank = generators.shape
    plan = Plan(rows_n, cols_n, rows_local, cols_local, block, rank, blocks)
    halves, row_cap, col_cap, half = plan.halves, plan.row_cap, plan.col_cap, plan.half_cap
    dt = generators.dtype
    parts = width // LANES
    table = pltpu.SMEM((plan.window,), jnp.int32)
    turns = range(1, halves)

    def shape(*lead):
        return jax.ShapeDtypeStruct(lead + (block, rank), dt)

    unit = jax.ShapeDtypeStruct((plan.unit, rank), dt)
    joined = jax.ShapeDtypeStruct((2, half * block, rank), dt)

    def sems(n):
        return pltpu.SemaphoreType.DMA((n,))

    def call(kernel, out_shape, in_specs, out_specs, scratch, mib, args, aliases={}):
        return pl.pallas_call(
            functools.partial(kernel, plan), out_shape=out_shape, in_specs=in_specs,
            out_specs=out_specs, scratch_shapes=scratch,
            input_output_aliases=aliases,
            compiler_params=pltpu.CompilerParams(vmem_limit_bytes=mib << 20))(*args)

    front = parent_front.reshape(rows_local, block, cols_local, parts, LANES)
    front = front.transpose(0, 1, 3, 2, 4).reshape(rows_local, block * plan.step, LANES)
    block_map, valid_rows, generators, diagonal_blocks, coupling, front = map(
        in_hbm, (block_map, valid_rows, generators, diagonal_blocks, coupling, front))

    def strip(n):
        return jax.ShapeDtypeStruct((n,) + front.shape[1:], front.dtype)

    def send(x, move):
        pairs = [
            (row * cols_n + col, to_row * cols_n + to_col)
            for row in range(rows_n)
            for col in range(cols_n)
            for to_row, to_col in [move(row, col)]
        ]
        return lax.ppermute(x, ("row", "col"), pairs)

    def across(d, k):
        return lambda row, col: (2 * ((row // 2 - d) % halves) + (row % 2 + k) % 2, col)

    def partner(row, col):
        return row ^ 1, col

    def beside(row, col):
        return row, col ^ 1

    def along(row, col):
        return row, col ^ halves

    flows = [(d, k) for d in turns for k in range(2)]
    maps = [pltpu.SMEM(block_map.shape, jnp.int32)] * 2 + [table] * 2
    every, mixers, *rows_out = call(
        pack_rows_kernel, [shape(blocks), shape(2)] + [unit] * len(flows), [ANY] * 4,
        [VMEM] * (2 + len(flows)), maps + [sems(4)], 8,
        (block_map, valid_rows, generators, coupling))
    near, beside_, along_, far_ = {}, {}, {}, {}
    for (d, k), x in zip(flows, rows_out):
        near[d, k] = send(x, across(d, k))
    mine, own, base, *sent = call(
        pack_rest_kernel,
        [shape(row_cap + 2 * col_cap), shape(row_cap), strip(row_cap)]
        + [unit] * (halves - 1) + [shape(col_cap)] * (halves - 1),
        [ANY, ANY, VMEM, VMEM, ANY, ANY], [VMEM] * (2 * halves + 1), maps + [sems(3 + col_cap)], 12,
        (block_map, valid_rows, every, mixers, diagonal_blocks, front))
    far_outs, cols_out = sent[: halves - 1], sent[halves - 1:]
    direct = {d: send(cols_out[d - 1], across(d, 0)) for d in turns}
    theirs = send(mine, partner)
    for d, k in flows:
        beside_[d, k] = send(near[d, k], beside)
        along_[d, k] = send(near[d, k], along)
    for d in turns:
        far_[d, 0] = send(beside_[d, 0], along)
        far_[d, 1] = send(far_outs[d - 1], across(d, 1))
    others = rows_local - row_cap
    rest = call(load_kernel, strip(others), [ANY], VMEM, [sems(others * PIECES)], 12, (front,))
    args = (own, mine, theirs, base)
    near_rows = call(begin_kernel, strip(row_cap), [VMEM] * 4, VMEM, [], 12, args)
    args = (mixers,) + tuple(direct[d] for d in turns) + tuple(
        x[flow] for flow in flows for x in (near, beside_))
    formed, leave, *fars = call(
        project_kernel, [shape(halves - 1, 2, col_cap)] * 2 + [joined] * (halves - 1),
        [VMEM] * len(args), [VMEM] * (1 + halves), [], 12, args)
    swapped = send(leave, partner)
    args = (mine, theirs, *fars, rest)
    even = call(even_kernel, strip(others // 2), [VMEM] * len(args), VMEM, [], 12, args)
    args = (own, mine, theirs, formed, swapped, *(direct[d] for d in turns), *fars) + tuple(
        x[flow] for flow in flows for x in (along_, far_)) + (base, rest, near_rows, even)
    n = len(args)
    out, _, _ = call(
        finish_kernel, [strip(rows_local), strip(row_cap), strip(others // 2)],
        [VMEM] * n, [ANY] + [VMEM] * 2,
        [pltpu.VMEM((others // 2,) + front.shape[1:], front.dtype), pltpu.VMEM(joined.shape, dt),
         pltpu.VMEM((halves, 2, col_cap, block, rank), dt), sems(rows_local * PIECES)],
        16, args, {n - 2: 1, n - 1: 2})
    out = out.reshape(rows_local, block, parts, cols_local, LANES)
    return out.transpose(0, 1, 3, 2, 4).reshape(rows_local, block, cols_local, width)


def solution(mesh):
    in_specs = (
        P(None, "row", None, "col"),
        P("row", None, None),
        P("row", None, None),
        P(),
        P(),
        P(),
    )
    out_specs = P(None, "row", None, "col")

    def body(*args):
        return shards(mesh.shape["row"], mesh.shape["col"], *args)

    return jax.shard_map(body, mesh=mesh, in_specs=in_specs, out_specs=out_specs, check_vma=False)
```

```python
import functools

import jax
import jax.numpy as jnp
from jax import lax
from jax.experimental import pallas as pl
from jax.experimental.pallas import tpu as pltpu
from jax.sharding import PartitionSpec as P


ANY = pl.BlockSpec(memory_space=pl.ANY)
SMEM = pl.BlockSpec(memory_space=pltpu.SMEM)
VMEM = pl.BlockSpec(memory_space=pltpu.VMEM)
LANES = 128
COST = 4 * 10**9
PIECES = 1


def in_hbm(x):
    return pltpu.with_memory_space_constraint(x, pltpu.HBM)


def in_vmem(x):
    return pltpu.with_memory_space_constraint(x, pltpu.VMEM)


class Plan:
    def __init__(self, rows_n, cols_n, rows_local, cols_local, block, rank, blocks):
        self.rows_n, self.cols_n = rows_n, cols_n
        self.halves = rows_n // 2
        self.window = 2 * rows_local
        self.rows_local, self.cols_local = rows_local, cols_local
        self.row_cap = self.window // rows_n
        self.col_cap = self.window // cols_n
        self.half_cap = self.row_cap // 2
        self.unit = self.half_cap * block // 2
        self.block, self.rank, self.blocks = block, rank, blocks
        self.step = cols_local * (block // LANES)
        assert cols_n == 2 * rows_n and self.half_cap == self.col_cap

    def here(self):
        row, col = lax.axis_index("row"), lax.axis_index("col")
        return row, col, row // 2, row % 2

    def parity(self, group, col):
        return (col // self.rows_n + (col // self.halves) % 2 + 2 * group // self.halves) % 2

    def owns_diag(self, group, col):
        return (col % self.rows_n) // 2 == group


def read_map(plan, block_map, valid_rows, child, group, count, where=None):
    for slot in range(plan.window):
        count[slot] = 0
        if where is not None:
            where[slot] = 0
    for i in range(plan.blocks):
        spot = block_map[child, group * plan.blocks + i] - group * plan.window
        count[spot] = valid_rows[child, group * plan.blocks + i]
        if where is not None:
            where[spot] = i


def keep_rows(x, count, start=0):
    pos = lax.broadcasted_iota(jnp.int32, (x.shape[0], 1), 0) + start
    return jnp.where(pos < count, x, jnp.zeros_like(x))


def keep_both(x, count):
    pos = lax.broadcasted_iota(jnp.int32, (1, x.shape[1]), 1)
    return jnp.where(pos < count, keep_rows(x, count), jnp.zeros_like(x))


def matmul(x, y):
    return jnp.dot(x, y, preferred_element_type=jnp.float32)


def project(x, mixer):
    dims = (((0,), (1,)), ((), ()))
    return lax.dot_general(mixer, x, dims, preferred_element_type=jnp.float32).astype(x.dtype)


def fill_unit(plan, out, every, where, count, target, parity, side):
    whole = plan.unit // plan.block
    for j in range(max(whole, 1)):
        slot = (2 * (side * whole + j) + parity) * plan.rows_n + target
        if whole:
            out[pl.ds(j * plan.block, plan.block), :] = keep_rows(every[where[slot]], count[slot])
        else:
            start = pl.multiple_of(side * plan.unit, plan.unit)
            part = every[where[slot], pl.ds(start, plan.unit), :]
            out[...] = keep_rows(part, count[slot], start)


def pack_rows_kernel(plan, block_map, valid_rows, generators, coupling, every, mixers, *refs):
    outs, (map_s, valid_s, where, count, sems) = refs[:-5], refs[-5:]
    _, col, group, child = plan.here()
    copies = [
        pltpu.make_async_copy(source, target, sems.at[i])
        for i, (source, target) in enumerate(
            ((generators, every), (block_map, map_s), (valid_rows, valid_s), (coupling, mixers)))
    ]
    for copy in copies:
        copy.start()
    copies[1].wait()
    copies[2].wait()
    read_map(plan, map_s, valid_s, child, group, count, where)
    copies[0].wait()
    side = col % 2
    for i, out in enumerate(outs):
        d, k = 1 + i // 2, i % 2
        aim = (group + plan.halves - d) % plan.halves
        fill_unit(plan, out, every, where, count, 2 * aim + (child + k) % 2, plan.parity(aim, col), side)
    copies[3].wait()


def pack_rest_kernel(plan, block_map, valid_rows, every, mixers, diagonal, front,
                     mine, own, base, *refs):
    turns = plan.halves - 1
    far_outs, outs, (map_s, valid_s, where, count, sems) = refs[:turns], refs[turns:-5], refs[-5:]
    row, col, group, child = plan.here()
    diags = plan.row_cap + plan.col_cap
    copies = [
        pltpu.make_async_copy(source, target, sems.at[i])
        for i, (source, target) in enumerate(
            ((block_map, map_s), (valid_rows, valid_s),
             (front.at[pl.ds(group * plan.row_cap, plan.row_cap)], base)))
    ]
    for copy in copies:
        copy.start()
    copies[0].wait()
    copies[1].wait()
    read_map(plan, map_s, valid_s, child, group, count, where)
    loads = []
    for s in range(plan.col_cap):
        source = diagonal.at[where[s * plan.cols_n + col]]
        loads.append(pltpu.make_async_copy(source, mine.at[diags + s], sems.at[3 + s]))
        loads[-1].start()
    for s in range(plan.col_cap):
        slot = s * plan.cols_n + col
        masked = keep_rows(every[where[slot]], count[slot])
        mine[plan.row_cap + s] = project(masked, mixers[child])
    for target, to in ((mine, 2 * group + (child + 1) % 2), (own, row)):
        for q in range(plan.row_cap):
            slot = q * plan.rows_n + to
            target[q] = keep_rows(every[where[slot]], count[slot])
    for i, out in enumerate(far_outs):
        aim = (group + plan.halves - (i + 1)) % plan.halves
        fill_unit(plan, out, every, where, count, 2 * aim + (child + 1) % 2,
                  1 - plan.parity(aim, col), 1 - col % 2)
    for s in range(plan.col_cap):
        loads[s].wait()
        mine[diags + s] = keep_both(mine[diags + s], count[s * plan.cols_n + col])
    for i, out in enumerate(outs):
        aim = (group + plan.halves - (i + 1)) % plan.halves
        owns = plan.owns_diag(aim, col)

        @pl.when(owns)
        def _():
            for s in range(plan.col_cap):
                out[s] = mine[diags + s]

        @pl.when(jnp.logical_not(owns))
        def _():
            for s in range(plan.col_cap):
                out[s] = mine[plan.row_cap + s]

    copies[2].wait()


def join(plan, target, k, here, there, side):
    first = pl.multiple_of(side * plan.unit, plan.unit)
    second = pl.multiple_of((1 - side) * plan.unit, plan.unit)
    target[k, pl.ds(first, plan.unit), :] = here[...]
    target[k, pl.ds(second, plan.unit), :] = there[...]


def project_kernel(plan, coupling, *refs):
    turns = plan.halves - 1
    directs, refs = refs[:turns], refs[turns:]
    parts, (formed, leave), fars = refs[: 4 * turns], refs[4 * turns: 4 * turns + 2], refs[4 * turns + 2:]
    row, col, _, child = plan.here()
    main = row == col % plan.rows_n
    for d in range(1, plan.halves):
        for k in range(2):
            here, there = parts[4 * (d - 1) + 2 * k: 4 * (d - 1) + 2 * k + 2]
            join(plan, fars[d - 1], k, here, there, col % 2)

    @pl.when(main)
    def _():
        for d in range(1, plan.halves):
            for k in range(2):
                mixer = coupling[(child + k) % 2]
                for j in range(plan.half_cap):
                    rows = fars[d - 1][k, pl.ds(j * plan.block, plan.block), :]
                    value = project(rows, mixer)
                    formed[d - 1, k, j] = value
                    leave[d - 1, k, j] = value

    @pl.when(jnp.logical_not(main))
    def _():
        for d in range(1, plan.halves):
            for j in range(plan.half_cap):
                leave[d - 1, 0, j] = directs[d - 1][j]


def put_across(plan, base, from_a, total, a, b, value):
    for part in range(plan.block // LANES):
        rows = pl.ds(part * plan.cols_local + b, plan.block, stride=plan.step)
        total[a, rows, :] = base[from_a, rows, :] + value[:, part * LANES:(part + 1) * LANES]


def put_tile(plan, base, total, a, b, value):
    put_across(plan, base, a, total, a, b, value)


def put_tiles(plan, base, total, steps, b, value):
    for j, a in enumerate(steps):
        put_tile(plan, base, total, a, b, value[j * plan.block:(j + 1) * plan.block])


def in_pieces(source, target, sems, copies):
    step = source.shape[0] // PIECES
    for i in range(PIECES):
        part = pl.ds(i * step, step)
        copies.append(pltpu.make_async_copy(source.at[part], target.at[part], sems.at[len(copies)]))
        copies[-1].start()


def begin_kernel(plan, own, mine, theirs, base, total):
    row, col, group, _ = plan.here()
    rows = plan.row_cap * plan.block
    left = own[...].reshape(rows, plan.rank)
    right = theirs[pl.ds(0, plan.row_cap)].reshape(rows, plan.rank)
    for s in range(plan.col_cap):
        value = matmul(left, mine[plan.row_cap + s]) + matmul(right, theirs[plan.row_cap + s])
        put_tiles(plan, base, total, range(plan.row_cap), group * plan.col_cap + s, value)

    @pl.when(row == col % plan.rows_n)
    def _():
        for s in range(plan.col_cap):
            slot = plan.row_cap + plan.col_cap + s
            value = mine[slot].astype(jnp.float32) + theirs[slot].astype(jnp.float32)
            put_tile(plan, total, total, 2 * s + col // plan.rows_n, group * plan.col_cap + s, value)


def even_kernel(plan, mine, theirs, *refs):
    fars, (front, even) = refs[:-2], refs[-2:]
    half = plan.half_cap
    _, col, group, _ = plan.here()
    parity = plan.parity(group, col)
    for d in range(1, plan.halves):
        far = fars[d - 1]
        for s in range(plan.col_cap):
            value = matmul(far[0], mine[plan.row_cap + s]) + matmul(far[1], theirs[plan.row_cap + s])
            for j in range(half):
                put_across(plan, front, (group + d) % plan.halves * plan.row_cap + 2 * j + parity,
                           even, (d - 1) * half + j, group * plan.col_cap + s,
                           value[j * plan.block:(j + 1) * plan.block])


def finish_kernel(plan, own, mine, theirs, formed, swapped, *refs):
    halves, half, turns = plan.halves, plan.half_cap, plan.halves - 1
    directs, fars, parts = refs[:turns], refs[turns: 2 * turns], refs[2 * turns: 6 * turns]
    base, front, _, _, out, near, even, odd, far, right, sems = refs[6 * turns:]
    row, col, group, _ = plan.here()
    owns = plan.owns_diag(group, col)
    main = row == col % plan.rows_n

    def choose(pick):
        for e in range(1, halves):
            for k in range(2):
                for s in range(plan.col_cap):
                    right[e, k, s] = pick(e - 1, k, s)

    @pl.when(main)
    def _():
        choose(lambda e, k, s: formed[e, k, s])

    @pl.when(owns & jnp.logical_not(main))
    def _():
        choose(lambda e, k, s: swapped[e, 1 - k, s])

    @pl.when(jnp.logical_not(owns))
    def _():
        choose(lambda e, k, s: swapped[e, 0, s] if k else directs[e][s])

    copies = []

    def rights(e, k, s):
        return right[e, k, s] if e else (mine, theirs)[k][plan.row_cap + s]

    def write(source, a):
        in_pieces(source, out.at[a], sems, copies)

    def spread(left, start, source, sources, total, places, first):
        rows = pl.ds(start, len(places) * plan.block)
        for e in range(first, halves):
            for s in range(plan.col_cap):
                value = matmul(left(0, rows), rights(e, 0, s)) + matmul(left(1, rows), rights(e, 1, s))
                b = (group + e) % halves * plan.col_cap + s
                for j, (a, place) in enumerate(zip(sources, places)):
                    put_across(plan, source, a, total, place, b,
                               value[j * plan.block:(j + 1) * plan.block])

    for q in range(plan.row_cap):
        spread(lambda k, rows: (own, theirs)[k][q], 0, base, [q], near, [q], 1)
        write(near.at[q], group * plan.row_cap + q)
    parity = plan.parity(group, col)
    for d in range(1, halves):
        places = range((d - 1) * half, d * half)
        top = (group + d) % halves * plan.row_cap

        @pl.when(row >= 0)
        def _():
            spread(lambda k, rows: fars[d - 1][k], 0, front,
                   [top + 2 * j + parity for j in range(half)], even, places, 1)

        @pl.when(main)
        def _():
            for s in range(plan.col_cap):
                value = directs[d - 1][s].astype(jnp.float32) + swapped[d - 1, 0, s].astype(jnp.float32)
                put_tile(plan, even, even, places[s], (group + d) % halves * plan.col_cap + s, value)

        for j in range(half):
            write(even.at[places[j]], top + 2 * j + parity)
        for k in range(2):
            here, there = parts[4 * (d - 1) + 2 * k: 4 * (d - 1) + 2 * k + 2]
            join(plan, far, k, here, there, col % 2)
        for j in range(half):
            spread(lambda k, rows: far[k, rows, :], j * plan.block, front,
                   [top + 2 * j + 1 - parity], odd, [places[j]], 0)
            write(odd.at[places[j]], top + 2 * j + 1 - parity)
    for copy in copies:
        copy.wait()


def shards(rows_n, cols_n, parent_front, generators, diagonal_blocks, coupling, block_map, valid_rows):
    rows_local, block, cols_local, width = parent_front.shape
    blocks, _, rank = generators.shape
    plan = Plan(rows_n, cols_n, rows_local, cols_local, block, rank, blocks)
    halves, row_cap, col_cap, half = plan.halves, plan.row_cap, plan.col_cap, plan.half_cap
    dt = generators.dtype
    parts = width // LANES
    table = pltpu.SMEM((plan.window,), jnp.int32)
    turns = range(1, halves)

    def shape(*lead):
        return jax.ShapeDtypeStruct(lead + (block, rank), dt)

    unit = jax.ShapeDtypeStruct((plan.unit, rank), dt)
    joined = jax.ShapeDtypeStruct((2, half * block, rank), dt)

    def sems(n):
        return pltpu.SemaphoreType.DMA((n,))

    def call(kernel, out_shape, in_specs, out_specs, scratch, mib, args, aliases={}):
        return pl.pallas_call(
            functools.partial(kernel, plan), out_shape=out_shape, in_specs=in_specs,
            out_specs=out_specs, scratch_shapes=scratch,
            input_output_aliases=aliases,
            cost_estimate=pl.CostEstimate(flops=COST, bytes_accessed=1 << 20, transcendentals=0),
            compiler_params=pltpu.CompilerParams(vmem_limit_bytes=mib << 20))(*args)

    front = parent_front.reshape(rows_local, block, cols_local, parts, LANES)
    front = front.transpose(0, 1, 3, 2, 4).reshape(rows_local, block * plan.step, LANES)
    block_map, valid_rows, generators, diagonal_blocks, coupling, front = map(
        in_hbm, (block_map, valid_rows, generators, diagonal_blocks, coupling, front))

    def strip(n):
        return jax.ShapeDtypeStruct((n,) + front.shape[1:], front.dtype)

    def send(x, move):
        pairs = [
            (row * cols_n + col, to_row * cols_n + to_col)
            for row in range(rows_n)
            for col in range(cols_n)
            for to_row, to_col in [move(row, col)]
        ]
        return lax.ppermute(x, ("row", "col"), pairs)

    def across(d, k):
        return lambda row, col: (2 * ((row // 2 - d) % halves) + (row % 2 + k) % 2, col)

    def partner(row, col):
        return row ^ 1, col

    def beside(row, col):
        return row, col ^ 1

    def along(row, col):
        return row, col ^ halves

    flows = [(d, k) for d in turns for k in range(2)]
    maps = [pltpu.SMEM(block_map.shape, jnp.int32)] * 2 + [table] * 2
    every, mixers, *rows_out = call(
        pack_rows_kernel, [shape(blocks), shape(2)] + [unit] * len(flows), [ANY] * 4,
        [VMEM] * (2 + len(flows)), maps + [sems(4)], 8,
        (block_map, valid_rows, generators, coupling))
    near, beside_, along_, far_ = {}, {}, {}, {}
    for (d, k), x in zip(flows, rows_out):
        near[d, k] = send(x, across(d, k))
    mine, own, base, *sent = call(
        pack_rest_kernel,
        [shape(row_cap + 2 * col_cap), shape(row_cap), strip(row_cap)]
        + [unit] * (halves - 1) + [shape(col_cap)] * (halves - 1),
        [ANY, ANY, VMEM, VMEM, ANY, ANY], [VMEM] * (2 * halves + 1), maps + [sems(3 + col_cap)], 12,
        (block_map, valid_rows, every, mixers, diagonal_blocks, front))
    far_outs, cols_out = sent[: halves - 1], sent[halves - 1:]
    direct = {d: send(cols_out[d - 1], across(d, 0)) for d in turns}
    theirs = send(mine, partner)
    for d, k in flows:
        beside_[d, k] = send(near[d, k], beside)
        along_[d, k] = send(near[d, k], along)
    for d in turns:
        far_[d, 0] = send(along_[d, 0], beside)
        far_[d, 1] = send(far_outs[d - 1], across(d, 1))
    others = rows_local - row_cap
    held = in_vmem(front)
    args = (own, mine, theirs, base)
    near_rows = call(begin_kernel, strip(row_cap), [VMEM] * 4, VMEM, [], 12, args)
    args = (mixers,) + tuple(direct[d] for d in turns) + tuple(
        x[flow] for flow in flows for x in (near, beside_))
    formed, leave, *fars = call(
        project_kernel, [shape(halves - 1, 2, col_cap)] * 2 + [joined] * (halves - 1),
        [VMEM] * len(args), [VMEM] * (1 + halves), [], 12, args)
    swapped = send(leave, partner)
    args = (mine, theirs, *fars, held)
    even = call(even_kernel, strip(others // 2), [VMEM] * len(args), VMEM, [], 12, args)
    args = (own, mine, theirs, formed, swapped, *(direct[d] for d in turns), *fars) + tuple(
        x[flow] for flow in flows for x in (along_, far_)) + (base, held, near_rows, even)
    n = len(args)
    out, _, _ = call(
        finish_kernel, [strip(rows_local), strip(row_cap), strip(others // 2)],
        [VMEM] * n, [ANY] + [VMEM] * 2,
        [pltpu.VMEM((others // 2,) + front.shape[1:], front.dtype), pltpu.VMEM(joined.shape, dt),
         pltpu.VMEM((halves, 2, col_cap, block, rank), dt), sems(rows_local * PIECES)],
        16, args, {n - 2: 1, n - 1: 2})
    out = out.reshape(rows_local, block, parts, cols_local, LANES)
    return out.transpose(0, 1, 3, 2, 4).reshape(rows_local, block, cols_local, width)


def solution(mesh):
    in_specs = (
        P(None, "row", None, "col"),
        P("row", None, None),
        P("row", None, None),
        P(),
        P(),
        P(),
    )
    out_specs = P(None, "row", None, "col")

    def body(*args):
        return shards(mesh.shape["row"], mesh.shape["col"], *args)

    return jax.shard_map(body, mesh=mesh, in_specs=in_specs, out_specs=out_specs, check_vma=False)
```

```python
import functools

import jax
import jax.numpy as jnp
from jax import lax
from jax.experimental import pallas as pl
from jax.experimental.pallas import tpu as pltpu
from jax.sharding import PartitionSpec as P


ANY = pl.BlockSpec(memory_space=pl.ANY)
SMEM = pl.BlockSpec(memory_space=pltpu.SMEM)
VMEM = pl.BlockSpec(memory_space=pltpu.VMEM)
LANES = 128
COST = 4 * 10**9
PIECES = 1


def in_hbm(x):
    return pltpu.with_memory_space_constraint(x, pltpu.HBM)


def in_vmem(x):
    return pltpu.with_memory_space_constraint(x, pltpu.VMEM)


class Plan:
    def __init__(self, rows_n, cols_n, rows_local, cols_local, block, rank, blocks):
        self.rows_n, self.cols_n = rows_n, cols_n
        self.halves = rows_n // 2
        self.window = 2 * rows_local
        self.rows_local, self.cols_local = rows_local, cols_local
        self.row_cap = self.window // rows_n
        self.col_cap = self.window // cols_n
        self.half_cap = self.row_cap // 2
        self.unit = self.half_cap * block // 2
        self.block, self.rank, self.blocks = block, rank, blocks
        self.step = cols_local * (block // LANES)
        assert cols_n == 2 * rows_n and self.half_cap == self.col_cap

    def here(self):
        row, col = lax.axis_index("row"), lax.axis_index("col")
        return row, col, row // 2, row % 2

    def parity(self, group, col):
        return (col // self.rows_n + (col // self.halves) % 2 + 2 * group // self.halves) % 2

    def owns_diag(self, group, col):
        return (col % self.rows_n) // 2 == group


def read_map(plan, block_map, valid_rows, child, group, count, where=None):
    for slot in range(plan.window):
        count[slot] = 0
        if where is not None:
            where[slot] = 0
    for i in range(plan.blocks):
        spot = block_map[child, group * plan.blocks + i] - group * plan.window
        count[spot] = valid_rows[child, group * plan.blocks + i]
        if where is not None:
            where[spot] = i


def keep_rows(x, count, start=0):
    pos = lax.broadcasted_iota(jnp.int32, (x.shape[0], 1), 0) + start
    return jnp.where(pos < count, x, jnp.zeros_like(x))


def keep_both(x, count):
    pos = lax.broadcasted_iota(jnp.int32, (1, x.shape[1]), 1)
    return jnp.where(pos < count, keep_rows(x, count), jnp.zeros_like(x))


def matmul(x, y):
    return jnp.dot(x, y, preferred_element_type=jnp.float32)


def project(x, mixer):
    dims = (((0,), (1,)), ((), ()))
    return lax.dot_general(mixer, x, dims, preferred_element_type=jnp.float32).astype(x.dtype)


def fill_unit(plan, out, every, where, count, target, parity, side):
    whole = plan.unit // plan.block
    for j in range(max(whole, 1)):
        slot = (2 * (side * whole + j) + parity) * plan.rows_n + target
        if whole:
            out[pl.ds(j * plan.block, plan.block), :] = keep_rows(every[where[slot]], count[slot])
        else:
            start = pl.multiple_of(side * plan.unit, plan.unit)
            part = every[where[slot], pl.ds(start, plan.unit), :]
            out[...] = keep_rows(part, count[slot], start)


def pack_rows_kernel(plan, block_map, valid_rows, generators, coupling, every, mixers, *refs):
    outs, (map_s, valid_s, where, count, sems) = refs[:-5], refs[-5:]
    _, col, group, child = plan.here()
    copies = [
        pltpu.make_async_copy(source, target, sems.at[i])
        for i, (source, target) in enumerate(
            ((generators, every), (block_map, map_s), (valid_rows, valid_s), (coupling, mixers)))
    ]
    for copy in copies:
        copy.start()
    copies[1].wait()
    copies[2].wait()
    read_map(plan, map_s, valid_s, child, group, count, where)
    copies[0].wait()
    side = col % 2
    for i, out in enumerate(outs):
        d, k = 1 + i // 2, i % 2
        aim = (group + plan.halves - d) % plan.halves
        fill_unit(plan, out, every, where, count, 2 * aim + (child + k) % 2, plan.parity(aim, col), side)
    copies[3].wait()


def pack_rest_kernel(plan, block_map, valid_rows, every, mixers, diagonal,
                     mine, own, *refs):
    turns = plan.halves - 1
    far_outs, outs, (map_s, valid_s, where, count, sems) = refs[:turns], refs[turns:-5], refs[-5:]
    row, col, group, child = plan.here()
    diags = plan.row_cap + plan.col_cap
    copies = [
        pltpu.make_async_copy(source, target, sems.at[i])
        for i, (source, target) in enumerate(
            ((block_map, map_s), (valid_rows, valid_s)))
    ]
    for copy in copies:
        copy.start()
    copies[0].wait()
    copies[1].wait()
    read_map(plan, map_s, valid_s, child, group, count, where)
    loads = []
    for s in range(plan.col_cap):
        source = diagonal.at[where[s * plan.cols_n + col]]
        loads.append(pltpu.make_async_copy(source, mine.at[diags + s], sems.at[2 + s]))
        loads[-1].start()
    for s in range(plan.col_cap):
        slot = s * plan.cols_n + col
        masked = keep_rows(every[where[slot]], count[slot])
        mine[plan.row_cap + s] = project(masked, mixers[child])
    for target, to in ((mine, 2 * group + (child + 1) % 2), (own, row)):
        for q in range(plan.row_cap):
            slot = q * plan.rows_n + to
            target[q] = keep_rows(every[where[slot]], count[slot])
    for i, out in enumerate(far_outs):
        aim = (group + plan.halves - (i + 1)) % plan.halves
        fill_unit(plan, out, every, where, count, 2 * aim + (child + 1) % 2,
                  1 - plan.parity(aim, col), 1 - col % 2)
    for s in range(plan.col_cap):
        loads[s].wait()
        mine[diags + s] = keep_both(mine[diags + s], count[s * plan.cols_n + col])
    for i, out in enumerate(outs):
        aim = (group + plan.halves - (i + 1)) % plan.halves
        owns = plan.owns_diag(aim, col)

        @pl.when(owns)
        def _():
            for s in range(plan.col_cap):
                out[s] = mine[diags + s]

        @pl.when(jnp.logical_not(owns))
        def _():
            for s in range(plan.col_cap):
                out[s] = mine[plan.row_cap + s]


def join(plan, target, k, here, there, side):
    first = pl.multiple_of(side * plan.unit, plan.unit)
    second = pl.multiple_of((1 - side) * plan.unit, plan.unit)
    target[k, pl.ds(first, plan.unit), :] = here[...]
    target[k, pl.ds(second, plan.unit), :] = there[...]


def project_kernel(plan, coupling, *refs):
    turns = plan.halves - 1
    directs, refs = refs[:turns], refs[turns:]
    parts, (formed, leave), fars = refs[: 4 * turns], refs[4 * turns: 4 * turns + 2], refs[4 * turns + 2:]
    row, col, _, child = plan.here()
    main = row == col % plan.rows_n
    for d in range(1, plan.halves):
        for k in range(2):
            here, there = parts[4 * (d - 1) + 2 * k: 4 * (d - 1) + 2 * k + 2]
            join(plan, fars[d - 1], k, here, there, col % 2)

    @pl.when(main)
    def _():
        for d in range(1, plan.halves):
            for k in range(2):
                mixer = coupling[(child + k) % 2]
                for j in range(plan.half_cap):
                    rows = fars[d - 1][k, pl.ds(j * plan.block, plan.block), :]
                    value = project(rows, mixer)
                    formed[d - 1, k, j] = value
                    leave[d - 1, k, j] = value

    @pl.when(jnp.logical_not(main))
    def _():
        for d in range(1, plan.halves):
            for j in range(plan.half_cap):
                leave[d - 1, 0, j] = directs[d - 1][j]


def put_across(plan, base, from_a, total, a, b, value):
    for part in range(plan.block // LANES):
        rows = pl.ds(part * plan.cols_local + b, plan.block, stride=plan.step)
        total[a, rows, :] = base[from_a, rows, :] + value[:, part * LANES:(part + 1) * LANES]


def put_tile(plan, base, total, a, b, value):
    put_across(plan, base, a, total, a, b, value)


def in_pieces(source, target, sems, copies):
    step = source.shape[0] // PIECES
    for i in range(PIECES):
        part = pl.ds(i * step, step)
        copies.append(pltpu.make_async_copy(source.at[part], target.at[part], sems.at[len(copies)]))
        copies[-1].start()


def begin_kernel(plan, own, mine, theirs, front, total):
    row, col, group, _ = plan.here()
    rows = plan.row_cap * plan.block
    left = own[...].reshape(rows, plan.rank)
    right = theirs[pl.ds(0, plan.row_cap)].reshape(rows, plan.rank)
    for s in range(plan.col_cap):
        value = matmul(left, mine[plan.row_cap + s]) + matmul(right, theirs[plan.row_cap + s])
        for q in range(plan.row_cap):
            put_across(plan, front, group * plan.row_cap + q, total, q, group * plan.col_cap + s,
                       value[q * plan.block:(q + 1) * plan.block])

    @pl.when(row == col % plan.rows_n)
    def _():
        for s in range(plan.col_cap):
            slot = plan.row_cap + plan.col_cap + s
            value = mine[slot].astype(jnp.float32) + theirs[slot].astype(jnp.float32)
            put_tile(plan, total, total, 2 * s + col // plan.rows_n, group * plan.col_cap + s, value)


def even_kernel(plan, mine, theirs, *refs):
    fars, (front, even) = refs[:-2], refs[-2:]
    half = plan.half_cap
    _, col, group, _ = plan.here()
    parity = plan.parity(group, col)
    for d in range(1, plan.halves):
        far = fars[d - 1]
        for s in range(plan.col_cap):
            value = matmul(far[0], mine[plan.row_cap + s]) + matmul(far[1], theirs[plan.row_cap + s])
            for j in range(half):
                put_across(plan, front, (group + d) % plan.halves * plan.row_cap + 2 * j + parity,
                           even, (d - 1) * half + j, group * plan.col_cap + s,
                           value[j * plan.block:(j + 1) * plan.block])


def finish_kernel(plan, own, mine, theirs, formed, swapped, *refs):
    halves, half, turns = plan.halves, plan.half_cap, plan.halves - 1
    directs, fars, parts = refs[:turns], refs[turns: 2 * turns], refs[2 * turns: 6 * turns]
    front, _, _, out, near, even, odd, far, right, sems = refs[6 * turns:]
    row, col, group, _ = plan.here()
    owns = plan.owns_diag(group, col)
    main = row == col % plan.rows_n

    def choose(pick):
        for e in range(1, halves):
            for k in range(2):
                for s in range(plan.col_cap):
                    right[e, k, s] = pick(e - 1, k, s)

    @pl.when(main)
    def _():
        choose(lambda e, k, s: formed[e, k, s])

    @pl.when(owns & jnp.logical_not(main))
    def _():
        choose(lambda e, k, s: swapped[e, 1 - k, s])

    @pl.when(jnp.logical_not(owns))
    def _():
        choose(lambda e, k, s: swapped[e, 0, s] if k else directs[e][s])

    copies = []

    def rights(e, k, s):
        return right[e, k, s] if e else (mine, theirs)[k][plan.row_cap + s]

    def write(source, a):
        in_pieces(source, out.at[a], sems, copies)

    def spread(left, start, source, sources, total, places, first):
        rows = pl.ds(start, len(places) * plan.block)
        for e in range(first, halves):
            for s in range(plan.col_cap):
                value = matmul(left(0, rows), rights(e, 0, s)) + matmul(left(1, rows), rights(e, 1, s))
                b = (group + e) % halves * plan.col_cap + s
                for j, (a, place) in enumerate(zip(sources, places)):
                    put_across(plan, source, a, total, place, b,
                               value[j * plan.block:(j + 1) * plan.block])

    for q in range(plan.row_cap):
        spread(lambda k, rows: (own, theirs)[k][q], 0, front,
               [group * plan.row_cap + q], near, [q], 1)
        write(near.at[q], group * plan.row_cap + q)
    parity = plan.parity(group, col)
    for d in range(1, halves):
        places = range((d - 1) * half, d * half)
        top = (group + d) % halves * plan.row_cap

        @pl.when(row >= 0)
        def _():
            spread(lambda k, rows: fars[d - 1][k], 0, front,
                   [top + 2 * j + parity for j in range(half)], even, places, 1)

        @pl.when(main)
        def _():
            for s in range(plan.col_cap):
                value = directs[d - 1][s].astype(jnp.float32) + swapped[d - 1, 0, s].astype(jnp.float32)
                put_tile(plan, even, even, places[s], (group + d) % halves * plan.col_cap + s, value)

        for j in range(half):
            write(even.at[places[j]], top + 2 * j + parity)
        for k in range(2):
            here, there = parts[4 * (d - 1) + 2 * k: 4 * (d - 1) + 2 * k + 2]
            join(plan, far, k, here, there, col % 2)
        for j in range(half):
            spread(lambda k, rows: far[k, rows, :], j * plan.block, front,
                   [top + 2 * j + 1 - parity], odd, [places[j]], 0)
            write(odd.at[places[j]], top + 2 * j + 1 - parity)
    for copy in copies:
        copy.wait()


def shards(rows_n, cols_n, parent_front, generators, diagonal_blocks, coupling, block_map, valid_rows):
    rows_local, block, cols_local, width = parent_front.shape
    blocks, _, rank = generators.shape
    plan = Plan(rows_n, cols_n, rows_local, cols_local, block, rank, blocks)
    halves, row_cap, col_cap, half = plan.halves, plan.row_cap, plan.col_cap, plan.half_cap
    dt = generators.dtype
    parts = width // LANES
    table = pltpu.SMEM((plan.window,), jnp.int32)
    turns = range(1, halves)

    def shape(*lead):
        return jax.ShapeDtypeStruct(lead + (block, rank), dt)

    unit = jax.ShapeDtypeStruct((plan.unit, rank), dt)
    joined = jax.ShapeDtypeStruct((2, half * block, rank), dt)

    def sems(n):
        return pltpu.SemaphoreType.DMA((n,))

    def call(kernel, out_shape, in_specs, out_specs, scratch, mib, args, aliases={}):
        return pl.pallas_call(
            functools.partial(kernel, plan), out_shape=out_shape, in_specs=in_specs,
            out_specs=out_specs, scratch_shapes=scratch,
            input_output_aliases=aliases,
            cost_estimate=pl.CostEstimate(flops=COST, bytes_accessed=1 << 20, transcendentals=0),
            compiler_params=pltpu.CompilerParams(vmem_limit_bytes=mib << 20))(*args)

    front = parent_front.reshape(rows_local, block, cols_local, parts, LANES)
    front = front.transpose(0, 1, 3, 2, 4).reshape(rows_local, block * plan.step, LANES)
    block_map, valid_rows, generators, diagonal_blocks, coupling, front = map(
        in_hbm, (block_map, valid_rows, generators, diagonal_blocks, coupling, front))

    def strip(n):
        return jax.ShapeDtypeStruct((n,) + front.shape[1:], front.dtype)

    def send(x, move):
        pairs = [
            (row * cols_n + col, to_row * cols_n + to_col)
            for row in range(rows_n)
            for col in range(cols_n)
            for to_row, to_col in [move(row, col)]
        ]
        return lax.ppermute(x, ("row", "col"), pairs)

    def across(d, k):
        return lambda row, col: (2 * ((row // 2 - d) % halves) + (row % 2 + k) % 2, col)

    def partner(row, col):
        return row ^ 1, col

    def beside(row, col):
        return row, col ^ 1

    def along(row, col):
        return row, col ^ halves

    flows = [(d, k) for d in turns for k in range(2)]
    held = in_vmem(front)
    maps = [pltpu.SMEM(block_map.shape, jnp.int32)] * 2 + [table] * 2
    every, mixers, *rows_out = call(
        pack_rows_kernel, [shape(blocks), shape(2)] + [unit] * len(flows), [ANY] * 4,
        [VMEM] * (2 + len(flows)), maps + [sems(4)], 8,
        (block_map, valid_rows, generators, coupling))
    near, beside_, along_, far_ = {}, {}, {}, {}
    for (d, k), x in zip(flows, rows_out):
        near[d, k] = send(x, across(d, k))
    mine, own, *sent = call(
        pack_rest_kernel,
        [shape(row_cap + 2 * col_cap), shape(row_cap)]
        + [unit] * (halves - 1) + [shape(col_cap)] * (halves - 1),
        [ANY, ANY, VMEM, VMEM, ANY], [VMEM] * (2 * halves), maps + [sems(2 + col_cap)], 12,
        (block_map, valid_rows, every, mixers, diagonal_blocks))
    far_outs, cols_out = sent[: halves - 1], sent[halves - 1:]
    direct = {d: send(cols_out[d - 1], across(d, 0)) for d in turns}
    theirs = send(mine, partner)
    for d, k in flows:
        beside_[d, k] = send(near[d, k], beside)
        along_[d, k] = send(near[d, k], along)
    for d in turns:
        far_[d, 0] = send(along_[d, 0], beside)
        far_[d, 1] = send(far_outs[d - 1], across(d, 1))
    others = rows_local - row_cap
    args = (own, mine, theirs, held)
    near_rows = call(begin_kernel, strip(row_cap), [VMEM] * 4, VMEM, [], 12, args)
    args = (mixers,) + tuple(direct[d] for d in turns) + tuple(
        x[flow] for flow in flows for x in (near, beside_))
    formed, leave, *fars = call(
        project_kernel, [shape(halves - 1, 2, col_cap)] * 2 + [joined] * (halves - 1),
        [VMEM] * len(args), [VMEM] * (1 + halves), [], 12, args)
    swapped = send(leave, partner)
    args = (mine, theirs, *fars, held)
    even = call(even_kernel, strip(others // 2), [VMEM] * len(args), VMEM, [], 12, args)
    args = (own, mine, theirs, formed, swapped, *(direct[d] for d in turns), *fars) + tuple(
        x[flow] for flow in flows for x in (along_, far_)) + (held, near_rows, even)
    n = len(args)
    out, _, _ = call(
        finish_kernel, [strip(rows_local), strip(row_cap), strip(others // 2)],
        [VMEM] * n, [ANY] + [VMEM] * 2,
        [pltpu.VMEM((others // 2,) + front.shape[1:], front.dtype), pltpu.VMEM(joined.shape, dt),
         pltpu.VMEM((halves, 2, col_cap, block, rank), dt), sems(rows_local * PIECES)],
        16, args, {n - 2: 1, n - 1: 2})
    out = out.reshape(rows_local, block, parts, cols_local, LANES)
    return out.transpose(0, 1, 3, 2, 4).reshape(rows_local, block, cols_local, width)


def solution(mesh):
    in_specs = (
        P(None, "row", None, "col"),
        P("row", None, None),
        P("row", None, None),
        P(),
        P(),
        P(),
    )
    out_specs = P(None, "row", None, "col")

    def body(*args):
        return shards(mesh.shape["row"], mesh.shape["col"], *args)

    return jax.shard_map(body, mesh=mesh, in_specs=in_specs, out_specs=out_specs, check_vma=False)
```
